256 devices in a mesh: slab: 8 (over z), pencil: 32 (over y, x, core).
Axes of the slice: x: 4, y: 4, z: 8, core: 2. Of those that a mesh axis runs over, the one named last changes fastest.
Arguments:
- right_sides: float32 [8, 128, 128, 128], P(None, 'slab', 'pencil'), may hold values from -6 to 6
- spectrum: float32 [128, 128, 128], P('pencil', 'slab'), may hold values from 0.5 to 20, as said below
- noise_var: float32 [128, 128, 128], P('slab', 'pencil'), may hold values from 0.05 to 1
- observed: int32 [128, 128, 128], P('slab', 'pencil'), may hold values 0 or 1
Outputs:
- solution: float32 [8, 128, 128, 128], P(None, 'slab', 'pencil')
- noise_grad: float32 [128, 128, 128], P('slab', 'pencil')
The draws below stay inside these ranges and needn't reach their ends.
Inputs may be any that keep to these rules, and one draw needn't show every extreme that they name: Even in every index: spectrum[a, b, c] equals spectrum[(-a) mod 128, (-b) mod 128, (-c) mod 128].
All inputs are finite; a program needn't handle non-finite values. No bound on the sum of `observed` on one device may be relied on, other than what follows from the above.
Results may differ from the reference program's by a relative error of at most 0.00021.
Values sent between devices are 32-bit elements; how exact they have to be, the bound alone decides.
No kernel may reach another device: no remote copies, remote signals or barrier semaphores. Data moves between devices by JAX's collectives and lax.ppermute only.
A program may use at most 64 MiB of HBM per device.

```python
import math
import jax
import jax.numpy as jnp
from jax import lax

NZ = 128
NY = 128
NX = 128
PROBES = 8
ITERS = 3


def draw_spectrum(key, part):
    base_values = jnp.exp(jax.random.uniform(key, (NX, NY, NZ), jnp.float32, math.log(0.5), math.log(20.0)))
    mirror = jnp.roll(jnp.flip(base_values, (0, 1, 2)), 1, (0, 1, 2))
    return 0.5 * (base_values + mirror)


def touch_ends(array, own_key, low, largest):
    extent = array.shape
    place = [jax.random.randint(jax.random.fold_in(own_key, axis), (), 0, extent[axis]) for axis in range(len(extent))]
    array = array.at[tuple(place)].set(low)
    longest = extent.index(max(extent))
    place[longest] = (place[longest] + 1) % extent[longest]
    return array.at[tuple(place)].set(largest)


def steps_of(own_key, extent, split, low, top_value):
    def one(position, parts):
        draws = jax.random.uniform(jax.random.fold_in(jax.random.fold_in(own_key, 6), position), (parts,), jnp.float32, low / len(split), top_value / len(split))
        return jnp.repeat(jnp.exp(draws), extent[position] // parts).reshape((-1,) + (1,) * (len(extent) - position - 1))

    factor_of = one(*split[0])
    for cut in split[1:]:
        factor_of = factor_of * one(*cut)
    return factor_of


def centred(rng, shape, deviation, reach, split=(), kind=jnp.bfloat16):
    factor_of = steps_of(rng, shape, split, -0.22, 0.18) if split else 1.0
    values = jax.random.normal(rng, shape, jnp.float32) * deviation * factor_of
    return jnp.minimum(jnp.maximum(values, -reach), reach).astype(kind)


def setup_inputs(seed: int = 0) -> dict:
    key_list = jax.random.split(jax.random.key(seed), 5)
    right_sides = centred(key_list[0], (PROBES, NZ, NY, NX), 1.0, 6.0, ((1, 8), (2, 32)), jnp.float32)
    spectrum = draw_spectrum(jax.random.fold_in(key_list[4], 71), 0)
    noise_var = jnp.clip(jnp.exp(math.log(1.0) - 2.9957323 * jax.random.uniform(key_list[2], (NZ, NY, NX), jnp.float32) ** steps_of(key_list[2], (NZ, NY, NX), ((0, 8), (1, 32)), -0.2, 0.2)), 0.05, 1.0)
    observed = touch_ends((jax.random.randint(key_list[3], (NZ, NY, NX), 0, 4) < 3).astype(jnp.int32), jax.random.fold_in(key_list[3], 1), 0, 1)
    return dict(right_sides=right_sides, spectrum=spectrum, noise_var=noise_var, observed=observed)


precise = lax.Precision.HIGHEST

def symmetric(matrix):
    return 0.5 * (matrix + matrix.T)

def solve_spd(matrix, right_hand):
    factor = jnp.linalg.cholesky(symmetric(matrix))
    halfway = lax.linalg.triangular_solve(factor, right_hand, left_side=True, lower=True)
    return lax.linalg.triangular_solve(factor, halfway, left_side=True, lower=True, transpose_a=True)

def gram_local(left, right):
    column_count = left.shape[0]
    return jnp.dot(left.reshape(column_count, -1), right.reshape(column_count, -1).T, precision=precise)

def combine(field_block, coefficients):
    column_count = field_block.shape[0]
    mixed = jnp.dot(coefficients.T, field_block.reshape(column_count, -1), precision=precise)
    return mixed.reshape(field_block.shape)

def operate(field_block, eigen_block, seen_cells, noise_var):
    masked = field_block * seen_cells
    spectral = jnp.fft.fftn(masked, axes=(1, 2, 3))
    smooth = jnp.real(jnp.fft.ifftn(spectral * eigen_block, axes=(1, 2, 3))).astype(jnp.float32)
    return seen_cells * smooth + noise_var * field_block

def reference(right_sides, spectrum, noise_var, observed):
    eigen_block = jnp.transpose(spectrum, (2, 1, 0))
    seen_cells = observed.astype(jnp.float32)
    solution = jnp.zeros_like(right_sides)
    residual = right_sides
    direction = right_sides
    gamma_now = gram_local(residual, residual)
    for iteration in range(ITERS):
        image_block = operate(direction, eigen_block, seen_cells, noise_var)
        delta_now = gram_local(direction, image_block)
        alpha_step = solve_spd(delta_now, gamma_now)
        solution = solution + combine(direction, alpha_step)
        if iteration + 1 < ITERS:
            residual = residual - combine(image_block, alpha_step)
            gamma_next = gram_local(residual, residual)
            beta_step = solve_spd(gamma_now, gamma_next)
            direction = residual + combine(direction, beta_step)
            gamma_now = gamma_next
    weights = right_sides[1:] * solution[1:]
    noise_grad = 0.5 * (solution[0] * solution[0] - jnp.mean(weights, axis=0))
    return (solution, noise_grad)
```

```python
import functools

import jax
import jax.numpy as jnp
import numpy as np
from jax import lax
from jax.experimental import pallas as pl
from jax.experimental.pallas import tpu as pltpu
from jax.sharding import PartitionSpec as P

GRID = 128
CELLS = GRID**3
COLUMNS = 8
SLABS = 8
PENCILS = 32
LINES = GRID // PENCILS
DEPTH = GRID // SLABS
ROWS = DEPTH * LINES
BLOCK = PENCILS * 4 * LINES
SHIFT = 6.0
WIDTH = 8.0
F32 = jnp.float32
BF16 = jnp.bfloat16


def slot_frequencies():
    first = np.where(np.arange(PENCILS) < PENCILS // 2, 0, 1)
    return np.arange(PENCILS)[:, None] * LINES + first[:, None] + np.arange(2)[None, :]


def split_table(table):
    high = table.astype(np.float32).astype(jnp.bfloat16)
    low = (table - high.astype(np.float64)).astype(np.float32).astype(jnp.bfloat16)
    return np.stack((high, low))


@functools.cache
def tables():
    points = np.arange(GRID)
    angle = 2.0 * np.pi / GRID * (points[:, None] * points[None, :] % GRID)
    cosine, sine = np.cos(angle), np.sin(angle)
    wave = slot_frequencies().reshape(-1)
    forward_x = np.stack((cosine[wave], -sine[wave]), axis=1)
    inverse_x = np.stack((2.0 * cosine[wave], -2.0 * sine[wave]), axis=1)
    forward_x[0, 1] = cosine[GRID // 2]
    inverse_x[0, 0] = 1.0
    inverse_x[0, 1] = cosine[GRID // 2]
    forward_x = forward_x.reshape(GRID, GRID)
    inverse_x = inverse_x.reshape(GRID, GRID) / (CELLS * WIDTH)
    forward = np.block([[cosine, sine], [-sine, cosine]])
    inverse = np.block([[cosine, -sine], [sine, cosine]])
    order = (
        np.arange(2)[None, :, None] * GRID
        + np.arange(PENCILS)[:, None, None] * LINES
        + np.arange(LINES)[None, None, :]
    ).reshape(-1)
    forward_y = forward[:, order]
    inverse_y = inverse[order, :]
    is_real = (order < GRID)[None, :]
    real_y = np.where(is_real, forward_y, 0.0)
    imag_y = np.where(is_real, 0.0, np.block([[cosine, cosine], [-sine, -sine]])[:, order])
    return (
        split_table(forward_x),
        split_table(inverse_x),
        np.stack([split_table(t) for t in (real_y, imag_y, forward_y, inverse_y)]),
        np.stack([split_table(t) for t in (forward.T, inverse.T)]),
    )


NN = (((1,), (0,)), ((), ()))
NT = (((1,), (1,)), ((), ()))
TN = (((0,), (0,)), ((), ()))


def halves(value):
    high = value.astype(BF16)
    return high, (value - high.astype(F32)).astype(BF16)


def product(left, right, dims):
    dot = functools.partial(lax.dot_general, dimension_numbers=dims, preferred_element_type=F32)
    return dot(left[0], right[0]) + (dot(left[0], right[1]) + dot(left[1], right[0]))


def pair(ref, *index):
    return ref[(*index, 0)], ref[(*index, 1)]


def lines_of(ref, line, start=0):
    return ref[:, pl.ds(start + line, DEPTH, stride=LINES), :].reshape(GRID, GRID)


def forward_x_lines(values, line, table_ref, out_ref):
    out_ref[pl.ds(line, GRID, stride=LINES), :] = product(pair(table_ref), halves(values), NT)


def start_kernel(staged_ref, table_ref, out_ref):
    for line in range(LINES):
        forward_x_lines(lines_of(staged_ref, line), line, table_ref, out_ref)


def spectrum_of(in_ref, slot, y_ref, z_ref, kind):
    block = in_ref[:, slot * 2 * LINES : (slot + 1) * 2 * LINES, :].reshape(2 * GRID, GRID)
    rows = product(pair(y_ref, kind), halves(block), NN)
    rows = jnp.concatenate((rows[:GRID], rows[GRID:]), axis=1)
    waves = product(halves(rows), pair(z_ref, 0), NN)
    return waves[:, :GRID], waves[:, GRID:]


def weighted_slots(in_ref, weights, y_ref, z_ref):
    real_weight, imag_weight, other_weight = weights
    real_re, real_im = spectrum_of(in_ref, 0, y_ref, z_ref, 0)
    imag_re, imag_im = spectrum_of(in_ref, 0, y_ref, z_ref, 1)
    other_re, other_im = spectrum_of(in_ref, 1, y_ref, z_ref, 2)
    return (
        (
            real_weight * real_re - imag_weight * imag_im,
            real_weight * real_im + imag_weight * imag_re,
        ),
        (other_weight * other_re, other_weight * other_im),
    )


def eigen_planes(staged_ref):
    return [
        staged_ref[:, 3 * ROWS + DEPTH * plane : 3 * ROWS + DEPTH * (plane + 1), :].reshape(
            GRID, GRID
        )
        for plane in range(3)
    ]


def middle_kernel(in_ref, staged_ref, y_ref, z_ref, out_ref):
    slots = weighted_slots(in_ref, eigen_planes(staged_ref), y_ref, z_ref)
    for slot, (real, imag) in enumerate(slots):
        waves = jnp.concatenate((real, imag), axis=1)
        rows = product(halves(waves), pair(z_ref, 1), NN)
        rows = jnp.concatenate((rows[:, :GRID], rows[:, GRID:]), axis=0)
        block = product(pair(y_ref, 3), halves(rows), NN)
        out_ref[:, slot * 2 * LINES : (slot + 1) * 2 * LINES, :] = block.reshape(
            PENCILS, 2 * LINES, GRID
        )


def back_kernel(in_ref, staged_ref, last_ref, inverse_ref, forward_ref, field_ref, out_ref):
    for line in range(LINES):
        waves = in_ref[pl.ds(line, GRID, stride=LINES), :]
        smooth = product(halves(waves), pair(inverse_ref), TN)
        seen = lines_of(staged_ref, line, ROWS)
        noise = lines_of(staged_ref, line, 2 * ROWS)
        field = seen * smooth + noise * lines_of(last_ref, line)
        field_ref[:, pl.ds(line, DEPTH, stride=LINES), :] = field.reshape(SLABS, DEPTH, GRID)
        forward_x_lines(field, line, forward_ref, out_ref)


def energy_kernel(in_ref, staged_ref, factor_ref, first_ref, second_ref, y_ref, z_ref, out_ref):
    planes = eigen_planes(staged_ref)
    factors = (factor_ref[0:1], factor_ref[0:1], factor_ref[1:2])
    weights = [jnp.sqrt(plane * factor) for plane, factor in zip(planes, factors)]
    slots = weighted_slots(in_ref, weights, y_ref, z_ref)
    for index, values in enumerate((*slots[0], *slots[1])):
        out_ref[:, index * DEPTH : (index + 1) * DEPTH, :] = values.reshape(SLABS, DEPTH, GRID)
    out_ref[:, ROWS : 2 * ROWS, :] = first_ref[:, :ROWS, :]
    out_ref[:, 2 * ROWS :, :] = second_ref[:, :ROWS, :]


def gram_kernel(in_ref, base_ref, seen_ref, noise_ref, first_ref, second_ref, out_ref):
    hidden = (1.0 - seen_ref[...]) * noise_ref[...]
    hidden_twice = hidden * noise_ref[...]
    for column in range(COLUMNS):
        source = column * 3 * ROWS
        rows = slice(column * ROWS, (column + 1) * ROWS)
        base = base_ref[rows, :]
        first_ref[rows, :] = in_ref[source + ROWS : source + 2 * ROWS, :] + hidden * base
        second_ref[rows, :] = in_ref[source + 2 * ROWS : source + 3 * ROWS, :] + hidden_twice * base
    zeroth, first, second, scaled, waves = [], [], [], [], []
    for row in range(ROWS):
        pick = pl.ds(row, COLUMNS, stride=ROWS)
        zeroth.append(base_ref[pick, :])
        first.append(first_ref[pick, :])
        second.append(second_ref[pick, :])
        scaled.append(second[-1] * noise_ref[row : row + 1, :])
        waves.append(in_ref[pl.ds(row, COLUMNS, stride=3 * ROWS), :])
    zeroth, first, second, scaled, waves = [
        halves(jnp.concatenate(parts, axis=1)) for parts in (zeroth, first, second, scaled, waves)
    ]
    out_ref[...] = jnp.zeros_like(out_ref)
    pairs = (
        (zeroth, zeroth),
        (zeroth, first),
        (first, first),
        (first, second),
        (second, second),
        (second, scaled),
        (waves, waves),
    )
    for index, (left, right) in enumerate(pairs):
        out_ref[:, index * COLUMNS : (index + 1) * COLUMNS] = product(left, right, NT)


def solve_kernel(
    sums_ref, base_ref, first_ref, second_ref, solution_ref, gradient_ref
):
    lanes = lax.broadcasted_iota(jnp.int32, (COLUMNS, GRID), 1)
    moments = sums_ref[0]
    for slab in range(1, SLABS):
        moments = moments + sums_ref[slab]
    last = (lanes >= 5 * COLUMNS) & (lanes < 6 * COLUMNS)
    moments = moments + jnp.where(last, pltpu.roll(moments, GRID - COLUMNS, 1), 0.0)

    def moved(count):
        return moments if count == 0 else pltpu.roll(moments, count * COLUMNS % GRID, 1)

    degree = 3
    size = degree * COLUMNS
    blocks = []
    for step in range(degree):
        operator = WIDTH * moved(GRID // COLUMNS - step - 1) + SHIFT * moved(
            (GRID // COLUMNS - step) % (GRID // COLUMNS)
        )
        blocks.append(jnp.where(lanes < size, operator, moved(degree - step)))
    system = jnp.concatenate(blocks, axis=0)
    rows = lax.broadcasted_iota(jnp.int32, (size, 1), 0)
    for step in range(size):
        pivot_row = system[step : step + 1, :]
        pivot_row = pivot_row / pivot_row[:, step : step + 1]
        reduced = system - system[:, step : step + 1] * pivot_row
        system = jnp.where(rows == step, pivot_row, reduced)
    sources = (base_ref, first_ref, second_ref)
    weighted = jnp.zeros((ROWS, GRID), F32)
    for target in range(COLUMNS):
        total = jnp.zeros((ROWS, GRID), F32)
        for index in range(size):
            block = sources[index // COLUMNS]
            column = index % COLUMNS
            coefficient = system[index : index + 1, size + target : size + target + 1]
            total = total + coefficient * block[column * ROWS : (column + 1) * ROWS, :]
        rows_out = slice(target * ROWS, (target + 1) * ROWS)
        solution_ref[rows_out, :] = total
        if target == 0:
            weighted = total * total
        else:
            share = 1.0 / (COLUMNS - 1)
            weighted = weighted - share * (total * base_ref[rows_out, :])
    gradient_ref[...] = 0.5 * weighted


def call(kernel, *shapes):
    outs = [jax.ShapeDtypeStruct(shape, F32) for shape in shapes]
    return pl.pallas_call(kernel, out_shape=outs if len(outs) > 1 else outs[0])


def exchange(values, axis, count):
    shape = values.shape
    parts = values.reshape(count, -1, shape[-1])
    return lax.all_to_all(parts, axis, 0, 0, tiled=True)


def own_planes(spectrum):
    pencil = lax.axis_index("pencil")
    low = pencil < PENCILS // 2
    first = jnp.where(low, spectrum[0], spectrum[1])
    second = jnp.where(low, spectrum[1], spectrum[2])
    middle = lax.ppermute(spectrum[0], "pencil", [(PENCILS // 2, 0)])
    partner = jnp.where(pencil == 0, middle, first)
    return jnp.stack((first, partner, second)).reshape(-1, GRID)


def local(right_sides, spectrum, noise_var, observed):
    forward_x, inverse_x, y_tables, z_tables = [jnp.asarray(t) for t in tables()]
    base = right_sides.reshape(COLUMNS, ROWS, GRID)
    seen = observed.astype(F32).reshape(ROWS, GRID)
    noise = (noise_var.reshape(ROWS, GRID) - SHIFT) * (1.0 / WIDTH)
    masked = base * seen
    extra = jnp.concatenate((seen, noise, own_planes(spectrum)), axis=0)
    extra = jnp.broadcast_to(extra[None], (SLABS, *extra.shape))
    staged = exchange(jnp.concatenate((masked, extra), axis=1), "slab", SLABS)

    flat = (BLOCK, GRID)
    cube = (SLABS, ROWS, GRID)
    sent = call(start_kernel, flat)(staged, forward_x)
    fields = [staged]
    for _ in range(2):
        parts = exchange(sent, "pencil", PENCILS)
        sent = call(middle_kernel, parts.shape)(parts, staged, y_tables, z_tables)
        parts = exchange(sent, "pencil", PENCILS).reshape(flat)
        field, sent = call(back_kernel, cube, flat)(
            parts, staged, fields[-1], inverse_x, forward_x
        )
        fields.append(field)
    parts = exchange(sent, "pencil", PENCILS)
    share = 2.0 / (CELLS * WIDTH)
    single = jnp.where(lax.axis_index("pencil") == 0, 0.5 * share, share)
    factors = jnp.broadcast_to(jnp.stack((single, jnp.float32(share)))[:, None], (2, GRID))
    merged = call(energy_kernel, (SLABS, 3 * ROWS, GRID))(
        parts, staged, factors, fields[1], fields[2], y_tables, z_tables
    )
    merged = exchange(merged, "slab", SLABS).reshape(-1, GRID)
    base = base.reshape(flat)
    first, second, sums = call(gram_kernel, flat, flat, (COLUMNS, GRID))(
        merged, base, seen, noise
    )
    sums = exchange(jnp.broadcast_to(sums[None], (PENCILS, COLUMNS, GRID)), "pencil", PENCILS)
    sums = jnp.sum(sums, axis=0)
    sums = exchange(jnp.broadcast_to(sums[None], (SLABS, COLUMNS, GRID)), "slab", SLABS)
    solution, gradient = call(solve_kernel, flat, (ROWS, GRID))(sums, base, first, second)
    return solution.reshape(right_sides.shape), gradient.reshape(noise_var.shape)


def solution(mesh):
    return jax.shard_map(
        local,
        mesh=mesh,
        in_specs=(
            P(None, "slab", "pencil", None),
            P("pencil", "slab", None),
            P("slab", "pencil", None),
            P("slab", "pencil", None),
        ),
        out_specs=(P(None, "slab", "pencil", None), P("slab", "pencil", None)),
        check_vma=False,
    )
```

```python
import functools

import jax
import jax.numpy as jnp
import numpy as np
from jax import lax
from jax.experimental import pallas as pl
from jax.experimental.pallas import tpu as pltpu
from jax.sharding import PartitionSpec as P

GRID = 128
CELLS = GRID**3
COLUMNS = 8
SLABS = 8
PENCILS = 32
LINES = GRID // PENCILS
DEPTH = GRID // SLABS
ROWS = DEPTH * LINES
BLOCK = PENCILS * 4 * LINES
SHIFT = 6.0
WIDTH = 8.0
F32 = jnp.float32
BF16 = jnp.bfloat16


def slot_frequencies():
    first = np.where(np.arange(PENCILS) < PENCILS // 2, 0, 1)
    return np.arange(PENCILS)[:, None] * LINES + first[:, None] + np.arange(2)[None, :]


def split_table(table):
    high = table.astype(np.float32).astype(jnp.bfloat16)
    low = (table - high.astype(np.float64)).astype(np.float32).astype(jnp.bfloat16)
    return np.stack((high, low))


@functools.cache
def tables():
    points = np.arange(GRID)
    angle = 2.0 * np.pi / GRID * (points[:, None] * points[None, :] % GRID)
    cosine, sine = np.cos(angle), np.sin(angle)
    wave = slot_frequencies().reshape(-1)
    forward_x = np.stack((cosine[wave], -sine[wave]), axis=1)
    inverse_x = np.stack((2.0 * cosine[wave], -2.0 * sine[wave]), axis=1)
    forward_x[0, 1] = cosine[GRID // 2]
    inverse_x[0, 0] = 1.0
    inverse_x[0, 1] = cosine[GRID // 2]
    forward_x = forward_x.reshape(GRID, GRID)
    inverse_x = inverse_x.reshape(GRID, GRID) / (CELLS * WIDTH)
    forward = np.block([[cosine, sine], [-sine, cosine]])
    inverse = np.block([[cosine, -sine], [sine, cosine]])
    order = (
        np.arange(2)[None, :, None] * GRID
        + np.arange(PENCILS)[:, None, None] * LINES
        + np.arange(LINES)[None, None, :]
    ).reshape(-1)
    forward_y = forward[:, order]
    inverse_y = inverse[order, :]
    is_real = (order < GRID)[None, :]
    real_y = np.where(is_real, forward_y, 0.0)
    imag_y = np.where(is_real, 0.0, np.block([[cosine, cosine], [-sine, -sine]])[:, order])
    return (
        split_table(forward_x),
        split_table(inverse_x),
        np.stack([split_table(t) for t in (real_y, imag_y, forward_y, inverse_y)]),
        np.stack([split_table(t) for t in (forward.T, inverse.T)]),
    )


NN = (((1,), (0,)), ((), ()))
NT = (((1,), (1,)), ((), ()))
TN = (((0,), (0,)), ((), ()))


def halves(value):
    high = value.astype(BF16)
    return high, (value - high.astype(F32)).astype(BF16)


def product(left, right, dims):
    dot = functools.partial(lax.dot_general, dimension_numbers=dims, preferred_element_type=F32)
    return dot(left[0], right[0]) + (dot(left[0], right[1]) + dot(left[1], right[0]))


def pair(ref, *index):
    return ref[(*index, 0)], ref[(*index, 1)]


def lines_of(ref, line, start=0):
    return ref[:, pl.ds(start + line, DEPTH, stride=LINES), :].reshape(GRID, GRID)


def forward_x_lines(values, line, table_ref, out_ref):
    out_ref[pl.ds(line, GRID, stride=LINES), :] = product(pair(table_ref), halves(values), NT)


def start_kernel(staged_ref, table_ref, out_ref):
    for line in range(LINES):
        forward_x_lines(lines_of(staged_ref, line), line, table_ref, out_ref)


def spectrum_of(in_ref, slot, y_ref, z_ref, kind):
    block = in_ref[:, slot * 2 * LINES : (slot + 1) * 2 * LINES, :].reshape(2 * GRID, GRID)
    rows = product(pair(y_ref, kind), halves(block), NN)
    rows = jnp.concatenate((rows[:GRID], rows[GRID:]), axis=1)
    waves = product(halves(rows), pair(z_ref, 0), NN)
    return waves[:, :GRID], waves[:, GRID:]


def weighted_slots(in_ref, weights, y_ref, z_ref):
    real_weight, imag_weight, other_weight = weights
    real_re, real_im = spectrum_of(in_ref, 0, y_ref, z_ref, 0)
    imag_re, imag_im = spectrum_of(in_ref, 0, y_ref, z_ref, 1)
    other_re, other_im = spectrum_of(in_ref, 1, y_ref, z_ref, 2)
    return (
        (
            real_weight * real_re - imag_weight * imag_im,
            real_weight * real_im + imag_weight * imag_re,
        ),
        (other_weight * other_re, other_weight * other_im),
    )


def plane_of(staged_ref, plane):
    start = 3 * ROWS + DEPTH * plane
    return staged_ref[:, start : start + DEPTH, :].reshape(GRID, GRID)


def eigen_planes(staged_ref, edge_ref):
    first = plane_of(staged_ref, 0)
    alone = lax.axis_index("pencil") == 0
    partner = jnp.where(alone, edge_ref[...], first)
    return alone, (first, partner, plane_of(staged_ref, 1))


def middle_kernel(in_ref, staged_ref, edge_ref, y_ref, z_ref, out_ref):
    slots = weighted_slots(in_ref, eigen_planes(staged_ref, edge_ref)[1], y_ref, z_ref)
    for slot, (real, imag) in enumerate(slots):
        waves = jnp.concatenate((real, imag), axis=1)
        rows = product(halves(waves), pair(z_ref, 1), NN)
        rows = jnp.concatenate((rows[:, :GRID], rows[:, GRID:]), axis=0)
        block = product(pair(y_ref, 3), halves(rows), NN)
        out_ref[:, slot * 2 * LINES : (slot + 1) * 2 * LINES, :] = block.reshape(
            PENCILS, 2 * LINES, GRID
        )


def back_kernel(in_ref, staged_ref, last_ref, inverse_ref, forward_ref, field_ref, out_ref):
    for line in range(LINES):
        waves = in_ref[pl.ds(line, GRID, stride=LINES), :]
        smooth = product(halves(waves), pair(inverse_ref), TN)
        seen = lines_of(staged_ref, line, ROWS)
        noise = lines_of(staged_ref, line, 2 * ROWS)
        field = seen * smooth + noise * lines_of(last_ref, line)
        field_ref[:, pl.ds(line, DEPTH, stride=LINES), :] = field.reshape(SLABS, DEPTH, GRID)
        forward_x_lines(field, line, forward_ref, out_ref)


def energy_kernel(in_ref, staged_ref, edge_ref, first_ref, second_ref, y_ref, z_ref, out_ref):
    alone, planes = eigen_planes(staged_ref, edge_ref)
    share = 2.0 / (CELLS * WIDTH)
    single = jnp.where(alone, 0.5 * share, share)
    factors = (single, single, share)
    weights = [jnp.sqrt(plane * factor) for plane, factor in zip(planes, factors)]
    slots = weighted_slots(in_ref, weights, y_ref, z_ref)
    for index, values in enumerate((*slots[0], *slots[1])):
        out_ref[:, index * DEPTH : (index + 1) * DEPTH, :] = values.reshape(SLABS, DEPTH, GRID)
    out_ref[:, ROWS : 2 * ROWS, :] = first_ref[:, :ROWS, :]
    out_ref[:, 2 * ROWS :, :] = second_ref[:, :ROWS, :]


def gram_kernel(in_ref, base_ref, seen_ref, noise_ref, first_ref, second_ref, out_ref):
    hidden = (1.0 - seen_ref[...]) * noise_ref[...]
    hidden_twice = hidden * noise_ref[...]
    for column in range(COLUMNS):
        source = column * 3 * ROWS
        rows = slice(column * ROWS, (column + 1) * ROWS)
        base = base_ref[rows, :]
        first_ref[rows, :] = in_ref[source + ROWS : source + 2 * ROWS, :] + hidden * base
        second_ref[rows, :] = in_ref[source + 2 * ROWS : source + 3 * ROWS, :] + hidden_twice * base
    zeroth, first, second, scaled, waves = [], [], [], [], []
    for row in range(ROWS):
        pick = pl.ds(row, COLUMNS, stride=ROWS)
        zeroth.append(base_ref[pick, :])
        first.append(first_ref[pick, :])
        second.append(second_ref[pick, :])
        scaled.append(second[-1] * noise_ref[row : row + 1, :])
        waves.append(in_ref[pl.ds(row, COLUMNS, stride=3 * ROWS), :])
    zeroth, first, second, scaled, waves = [
        halves(jnp.concatenate(parts, axis=1)) for parts in (zeroth, first, second, scaled, waves)
    ]
    out_ref[...] = jnp.zeros_like(out_ref)
    pairs = (
        (zeroth, zeroth),
        (zeroth, first),
        (first, first),
        (first, second),
        (second, second),
        (second, scaled),
        (waves, waves),
    )
    for index, (left, right) in enumerate(pairs):
        out_ref[:, index * COLUMNS : (index + 1) * COLUMNS] = product(left, right, NT)


def solve_kernel(
    sums_ref, base_ref, first_ref, second_ref, solution_ref, gradient_ref
):
    lanes = lax.broadcasted_iota(jnp.int32, (COLUMNS, GRID), 1)
    moments = sums_ref[0]
    for slab in range(1, SLABS):
        moments = moments + sums_ref[slab]
    last = (lanes >= 5 * COLUMNS) & (lanes < 6 * COLUMNS)
    moments = moments + jnp.where(last, pltpu.roll(moments, GRID - COLUMNS, 1), 0.0)

    def moved(count):
        return moments if count == 0 else pltpu.roll(moments, count * COLUMNS % GRID, 1)

    degree = 3
    size = degree * COLUMNS
    blocks = []
    for step in range(degree):
        operator = WIDTH * moved(GRID // COLUMNS - step - 1) + SHIFT * moved(
            (GRID // COLUMNS - step) % (GRID // COLUMNS)
        )
        blocks.append(jnp.where(lanes < size, operator, moved(degree - step)))
    system = jnp.concatenate(blocks, axis=0)
    rows = lax.broadcasted_iota(jnp.int32, (size, 1), 0)
    for step in range(size):
        pivot_row = system[step : step + 1, :]
        pivot_row = pivot_row / pivot_row[:, step : step + 1]
        reduced = system - system[:, step : step + 1] * pivot_row
        system = jnp.where(rows == step, pivot_row, reduced)
    sources = (base_ref, first_ref, second_ref)
    weighted = jnp.zeros((ROWS, GRID), F32)
    for target in range(COLUMNS):
        total = jnp.zeros((ROWS, GRID), F32)
        for index in range(size):
            block = sources[index // COLUMNS]
            column = index % COLUMNS
            coefficient = system[index : index + 1, size + target : size + target + 1]
            total = total + coefficient * block[column * ROWS : (column + 1) * ROWS, :]
        rows_out = slice(target * ROWS, (target + 1) * ROWS)
        solution_ref[rows_out, :] = total
        if target == 0:
            weighted = total * total
        else:
            share = 1.0 / (COLUMNS - 1)
            weighted = weighted - share * (total * base_ref[rows_out, :])
    gradient_ref[...] = 0.5 * weighted


def stage_kernel(base_ref, observed_ref, noise_ref, spectrum_ref, out_ref, seen_ref, shifted_ref):
    seen = observed_ref[...].astype(F32)
    shifted = (noise_ref[...] - SHIFT) * (1.0 / WIDTH)
    seen_ref[...] = seen
    shifted_ref[...] = shifted
    low = lax.axis_index("pencil") < PENCILS // 2
    first = jnp.where(low, spectrum_ref[0], spectrum_ref[1])
    second = jnp.where(low, spectrum_ref[1], spectrum_ref[2])
    parts = (seen, shifted, first, second, spectrum_ref[0])
    for slab in range(SLABS):
        out_ref[slab, :ROWS, :] = base_ref[slab] * seen
        start = ROWS
        for part in parts:
            out_ref[slab, start : start + part.shape[0], :] = part
            start += part.shape[0]


def call(kernel, *shapes, inputs=True, outputs=True):
    kind = pltpu.VMEM if outputs else jax.ShapeDtypeStruct
    outs = [kind(shape, F32) for shape in shapes]
    run = pl.pallas_call(
        kernel,
        out_shape=outs if len(outs) > 1 else outs[0],
        compiler_params=pltpu.CompilerParams(vmem_limit_bytes=24 * 2**20),
    )

    def placed(*values):
        if inputs:
            values = [pltpu.with_memory_space_constraint(value, pltpu.VMEM) for value in values]
        return run(*values)

    return placed


def exchange(values, axis, count):
    shape = values.shape
    parts = values.reshape(count, -1, shape[-1])
    return lax.all_to_all(parts, axis, 0, 0, tiled=True)


def local(right_sides, spectrum, noise_var, observed):
    forward_x, inverse_x, y_tables, z_tables = [jnp.asarray(t) for t in tables()]
    flat = (BLOCK, GRID)
    cube = (SLABS, ROWS, GRID)
    square = (ROWS, GRID)
    staged, seen, noise = call(
        stage_kernel, (SLABS, 3 * ROWS + 3 * DEPTH, GRID), square, square, inputs=False
    )(
        right_sides.reshape(cube),
        observed.reshape(square),
        noise_var.reshape(square),
        spectrum,
    )
    staged = exchange(staged, "slab", SLABS)
    edge = staged[:, 3 * ROWS + 2 * DEPTH :, :].reshape(GRID, GRID)
    edge = lax.ppermute(edge, "pencil", [(PENCILS // 2, 0)])

    sent = call(start_kernel, flat)(staged, forward_x)
    fields = [staged]
    for _ in range(2):
        parts = exchange(sent, "pencil", PENCILS)
        sent = call(middle_kernel, parts.shape)(parts, staged, edge, y_tables, z_tables)
        parts = exchange(sent, "pencil", PENCILS).reshape(flat)
        field, sent = call(back_kernel, cube, flat)(
            parts, staged, fields[-1], inverse_x, forward_x
        )
        fields.append(field)
    parts = exchange(sent, "pencil", PENCILS)
    merged = call(energy_kernel, (SLABS, 3 * ROWS, GRID))(
        parts, staged, edge, fields[1], fields[2], y_tables, z_tables
    )
    merged = exchange(merged, "slab", SLABS).reshape(-1, GRID)
    base = right_sides.reshape(flat)
    first, second, sums = call(gram_kernel, flat, flat, (COLUMNS, GRID))(
        merged, base, seen, noise
    )
    sums = exchange(jnp.broadcast_to(sums[None], (PENCILS, COLUMNS, GRID)), "pencil", PENCILS)
    sums = jnp.sum(sums, axis=0)
    sums = exchange(jnp.broadcast_to(sums[None], (SLABS, COLUMNS, GRID)), "slab", SLABS)
    solution, gradient = call(solve_kernel, flat, (ROWS, GRID), outputs=False)(
        sums, base, first, second
    )
    return solution.reshape(right_sides.shape), gradient.reshape(noise_var.shape)


def solution(mesh):
    return jax.shard_map(
        local,
        mesh=mesh,
        in_specs=(
            P(None, "slab", "pencil", None),
            P("pencil", "slab", None),
            P("slab", "pencil", None),
            P("slab", "pencil", None),
        ),
        out_specs=(P(None, "slab", "pencil", None), P("slab", "pencil", None)),
        check_vma=False,
    )
```

```python
import functools

import jax
import jax.numpy as jnp
import numpy as np
from jax import lax
from jax.experimental import pallas as pl
from jax.experimental.pallas import tpu as pltpu
from jax.sharding import PartitionSpec as P


GRID = 128
CELLS = GRID**3
COLUMNS = 8
SLABS = 8
PENCILS = 32
LINES = GRID // PENCILS
DEPTH = GRID // SLABS
ROWS = DEPTH * LINES
BLOCK = PENCILS * 4 * LINES
SHIFT = 6.0
WIDTH = 8.0
F32 = jnp.float32
BF16 = jnp.bfloat16


def slot_frequencies():
    first = np.where(np.arange(PENCILS) < PENCILS // 2, 0, 1)
    return np.arange(PENCILS)[:, None] * LINES + first[:, None] + np.arange(2)[None, :]


def split_table(table):
    high = table.astype(np.float32).astype(jnp.bfloat16)
    low = (table - high.astype(np.float64)).astype(np.float32).astype(jnp.bfloat16)
    return np.stack((high, low))


@functools.cache
def tables():
    points = np.arange(GRID)
    angle = 2.0 * np.pi / GRID * (points[:, None] * points[None, :] % GRID)
    cosine, sine = np.cos(angle), np.sin(angle)
    wave = slot_frequencies().reshape(-1)
    forward_x = np.stack((cosine[wave], -sine[wave]), axis=1)
    inverse_x = np.stack((2.0 * cosine[wave], -2.0 * sine[wave]), axis=1)
    forward_x[0, 1] = cosine[GRID // 2]
    inverse_x[0, 0] = 1.0
    inverse_x[0, 1] = cosine[GRID // 2]
    forward_x = forward_x.reshape(GRID, GRID)
    inverse_x = inverse_x.reshape(GRID, GRID) / (CELLS * WIDTH)
    forward = np.block([[cosine, sine], [-sine, cosine]])
    inverse = np.block([[cosine, -sine], [sine, cosine]])
    order = (
        np.arange(2)[None, :, None] * GRID
        + np.arange(PENCILS)[:, None, None] * LINES
        + np.arange(LINES)[None, None, :]
    ).reshape(-1)
    forward_y = forward[:, order]
    inverse_y = inverse[order, :]
    return (
        split_table(forward_x),
        split_table(inverse_x),
        np.stack([split_table(t) for t in (forward_y, inverse_y)]),
        np.stack([split_table(t) for t in (forward.T, inverse.T)]),
    )


NN = (((1,), (0,)), ((), ()))
NT = (((1,), (1,)), ((), ()))
TN = (((0,), (0,)), ((), ()))


def halves(value):
    high = value.astype(BF16)
    return high, (value - high.astype(F32)).astype(BF16)


def product(left, right, dims):
    dot = functools.partial(lax.dot_general, dimension_numbers=dims, preferred_element_type=F32)
    return dot(left[0], right[0]) + (dot(left[0], right[1]) + dot(left[1], right[0]))


def pair(ref, *index):
    return ref[(*index, 0)], ref[(*index, 1)]


def lines_of(ref, line, start=0):
    return ref[:, pl.ds(start + line, DEPTH, stride=LINES), :].reshape(GRID, GRID)


def forward_x_lines(values, line, table_ref, out_ref):
    out_ref[pl.ds(line, GRID, stride=LINES), :] = product(pair(table_ref), halves(values), NT)


def start_kernel(staged_ref, table_ref, out_ref):
    for line in range(LINES):
        forward_x_lines(lines_of(staged_ref, line), line, table_ref, out_ref)


def spectrum_of(block, y_ref, z_ref):
    rows = product(pair(y_ref, 0), halves(block), NN)
    rows = jnp.concatenate((rows[:GRID], rows[GRID:]), axis=1)
    return product(halves(rows), pair(z_ref, 0), NN)


def slot_of(in_ref, slot):
    return in_ref[:, slot * 2 * LINES : (slot + 1) * 2 * LINES, :].reshape(2 * GRID, GRID)


def weighted_slots(in_ref, weights, y_ref, z_ref):
    real_weight, imag_weight, other_weight = [
        jnp.concatenate((weight, weight), axis=1) for weight in weights
    ]
    block = slot_of(in_ref, 0)
    rows = lax.broadcasted_iota(jnp.int32, block.shape, 0)
    is_real = rows % (2 * LINES) < LINES
    real = spectrum_of(jnp.where(is_real, block, 0.0), y_ref, z_ref)
    imag = spectrum_of(jnp.where(is_real, 0.0, block), y_ref, z_ref)
    other = spectrum_of(slot_of(in_ref, 1), y_ref, z_ref)
    return real_weight * real + imag_weight * imag, other_weight * other


def plane_of(staged_ref, plane):
    start = ROWS + DEPTH * plane
    return staged_ref[:, start : start + DEPTH, :].reshape(GRID, GRID)


def eigen_planes(staged_ref, edge_ref):
    first = plane_of(staged_ref, 0)
    alone = lax.axis_index("pencil") == 0
    partner = jnp.where(alone, edge_ref[...], first)
    return alone, (first, partner, plane_of(staged_ref, 1))


def middle_kernel(in_ref, staged_ref, edge_ref, y_ref, z_ref, out_ref):
    slots = weighted_slots(in_ref, eigen_planes(staged_ref, edge_ref)[1], y_ref, z_ref)
    for slot, waves in enumerate(slots):
        rows = product(halves(waves), pair(z_ref, 1), NN)
        rows = jnp.concatenate((rows[:, :GRID], rows[:, GRID:]), axis=0)
        block = product(pair(y_ref, 1), halves(rows), NN)
        out_ref[:, slot * 2 * LINES : (slot + 1) * 2 * LINES, :] = block.reshape(
            PENCILS, 2 * LINES, GRID
        )


def neighbour(step):
    return lax.rem(lax.axis_index("slab") + (SLABS + step), SLABS)


def first_back_kernel(in_ref, last_ref, inverse_ref, forward_ref, *refs):
    parts, (mask_ref, field_ref, out_ref) = refs[:SLABS], refs[SLABS:]
    for step, part in enumerate(parts):
        mask_ref[neighbour(-step)] = part[...]
    back_kernel(in_ref, mask_ref, last_ref, inverse_ref, forward_ref, field_ref, out_ref)


def back_kernel(in_ref, mask_ref, last_ref, inverse_ref, forward_ref, field_ref, out_ref):
    for line in range(LINES):
        waves = in_ref[pl.ds(line, GRID, stride=LINES), :]
        smooth = product(halves(waves), pair(inverse_ref), TN)
        seen = lines_of(mask_ref, line)
        noise = lines_of(mask_ref, line, ROWS)
        field = seen * smooth + noise * lines_of(last_ref, line)
        field_ref[:, pl.ds(line, DEPTH, stride=LINES), :] = field.reshape(SLABS, DEPTH, GRID)
        forward_x_lines(field, line, forward_ref, out_ref)


def energy_kernel(in_ref, staged_ref, edge_ref, first_ref, second_ref, y_ref, z_ref, out_ref):
    alone, planes = eigen_planes(staged_ref, edge_ref)
    share = 2.0 / (CELLS * WIDTH)
    single = jnp.where(alone, 0.5 * share, share)
    factors = (single, single, share)
    weights = [jnp.sqrt(plane * factor) for plane, factor in zip(planes, factors)]
    slots = weighted_slots(in_ref, weights, y_ref, z_ref)
    for index in range(4):
        part = index % 2 * GRID
        values = slots[index // 2][:, part : part + GRID]
        out_ref[:, index * DEPTH : (index + 1) * DEPTH, :] = values.reshape(SLABS, DEPTH, GRID)
    out_ref[:, ROWS : 2 * ROWS, :] = first_ref[...]
    out_ref[:, 2 * ROWS :, :] = second_ref[...]


def gram_kernel(in_ref, base_ref, mask_ref, first_ref, second_ref, out_ref):
    noise_ref = mask_ref.at[ROWS:, :]
    hidden = (1.0 - mask_ref[:ROWS, :]) * noise_ref[...]
    hidden_twice = hidden * noise_ref[...]
    for column in range(COLUMNS):
        source = column * 3 * ROWS
        rows = slice(column * ROWS, (column + 1) * ROWS)
        base = base_ref[rows, :]
        first_ref[rows, :] = in_ref[source + ROWS : source + 2 * ROWS, :] + hidden * base
        second_ref[rows, :] = in_ref[source + 2 * ROWS : source + 3 * ROWS, :] + hidden_twice * base
    zeroth, first, second, scaled, waves = [], [], [], [], []
    for row in range(ROWS):
        pick = pl.ds(row, COLUMNS, stride=ROWS)
        zeroth.append(base_ref[pick, :])
        first.append(first_ref[pick, :])
        second.append(second_ref[pick, :])
        scaled.append(second[-1] * noise_ref[row : row + 1, :])
        waves.append(in_ref[pl.ds(row, COLUMNS, stride=3 * ROWS), :])
    zeroth, first, second, scaled, waves = [
        halves(jnp.concatenate(parts, axis=1)) for parts in (zeroth, first, second, scaled, waves)
    ]
    out_ref[...] = jnp.zeros_like(out_ref)
    pairs = (
        (zeroth, zeroth),
        (zeroth, first),
        (first, first),
        (first, second),
        (second, second),
        (second, scaled),
        (waves, waves),
    )
    for index, (left, right) in enumerate(pairs):
        out_ref[:, index * COLUMNS : (index + 1) * COLUMNS] = product(left, right, NT)


def solve_kernel(
    sums_ref, base_ref, first_ref, second_ref, solution_ref, gradient_ref
):
    lanes = lax.broadcasted_iota(jnp.int32, (COLUMNS, GRID), 1)
    moments = sums_ref[0]
    for slab in range(1, SLABS):
        moments = moments + sums_ref[slab]
    last = (lanes >= 5 * COLUMNS) & (lanes < 6 * COLUMNS)
    moments = moments + jnp.where(last, pltpu.roll(moments, GRID - COLUMNS, 1), 0.0)

    def moved(count):
        return moments if count == 0 else pltpu.roll(moments, count * COLUMNS % GRID, 1)

    degree = 3
    size = degree * COLUMNS
    blocks = []
    for step in range(degree):
        operator = WIDTH * moved(GRID // COLUMNS - step - 1) + SHIFT * moved(
            (GRID // COLUMNS - step) % (GRID // COLUMNS)
        )
        blocks.append(jnp.where(lanes < size, operator, moved(degree - step)))
    system = jnp.concatenate(blocks, axis=0)
    rows = lax.broadcasted_iota(jnp.int32, (size, 1), 0)
    for step in range(size):
        pivot_row = system[step : step + 1, :]
        pivot_row = pivot_row / pivot_row[:, step : step + 1]
        reduced = system - system[:, step : step + 1] * pivot_row
        system = jnp.where(rows == step, pivot_row, reduced)
    sources = (base_ref, first_ref, second_ref)
    weighted = jnp.zeros((ROWS, GRID), F32)
    for target in range(COLUMNS):
        total = jnp.zeros((ROWS, GRID), F32)
        for index in range(size):
            block = sources[index // COLUMNS]
            column = index % COLUMNS
            coefficient = system[index : index + 1, size + target : size + target + 1]
            total = total + coefficient * block[column * ROWS : (column + 1) * ROWS, :]
        rows_out = slice(target * ROWS, (target + 1) * ROWS)
        solution_ref[rows_out, :] = total
        if target == 0:
            weighted = total * total
        else:
            share = 1.0 / (COLUMNS - 1)
            weighted = weighted - share * (total * base_ref[rows_out, :])
    gradient_ref[...] = 0.5 * weighted


def stage_kernel(base_ref, observed_ref, noise_ref, spectrum_ref, out_ref, mask_ref):
    seen = observed_ref[...].astype(F32)
    mask_ref[:ROWS, :] = seen
    mask_ref[ROWS:, :] = (noise_ref[...] - SHIFT) * (1.0 / WIDTH)
    low = lax.axis_index("pencil") < PENCILS // 2
    first = jnp.where(low, spectrum_ref[0], spectrum_ref[1])
    second = jnp.where(low, spectrum_ref[1], spectrum_ref[2])
    for slab in range(SLABS):
        out_ref[slab, :ROWS, :] = base_ref[slab] * seen
        for index, plane in enumerate((first, second, spectrum_ref[0])):
            start = ROWS + index * DEPTH
            out_ref[slab, start : start + DEPTH, :] = plane


def call(kernel, *shapes, inputs=pltpu.VMEM, outputs=True):
    kind = pltpu.VMEM if outputs else jax.ShapeDtypeStruct
    outs = [kind(shape, F32) for shape in shapes]
    run = pl.pallas_call(
        kernel,
        out_shape=outs if len(outs) > 1 else outs[0],
        compiler_params=pltpu.CompilerParams(vmem_limit_bytes=24 * 2**20),
    )

    def placed(*values):
        return run(*[pltpu.with_memory_space_constraint(value, inputs) for value in values])

    return placed


def exchange(values, axis, count):
    shape = values.shape
    parts = values.reshape(count, -1, shape[-1])
    return lax.all_to_all(parts, axis, 0, 0, tiled=True)


def shifted(values, step):
    ring = [(slab, (slab + step) % SLABS) for slab in range(SLABS)]
    return lax.ppermute(values, "slab", ring)


def local(right_sides, spectrum, noise_var, observed):
    forward_x, inverse_x, y_tables, z_tables = [jnp.asarray(t) for t in tables()]
    flat = (BLOCK, GRID)
    cube = (SLABS, ROWS, GRID)
    square = (ROWS, GRID)
    double = (2 * ROWS, GRID)
    staged, mask = call(
        stage_kernel, (SLABS, ROWS + 3 * DEPTH, GRID), double, inputs=pltpu.HBM
    )(
        right_sides.reshape(cube),
        observed.reshape(square),
        noise_var.reshape(square),
        spectrum,
    )
    staged = exchange(staged, "slab", SLABS)
    edge = staged[:, ROWS + 2 * DEPTH :, :].reshape(GRID, GRID)
    edge = lax.ppermute(edge, "pencil", [(PENCILS // 2, 0)])
    masks = [mask]
    for step in range(1, SLABS):
        masks.append(shifted(mask, step))

    sent = call(start_kernel, flat)(staged, forward_x)
    parts = exchange(sent, "pencil", PENCILS)
    sent = call(middle_kernel, parts.shape)(parts, staged, edge, y_tables, z_tables)
    parts = exchange(sent, "pencil", PENCILS).reshape(flat)
    masks, field, sent = call(first_back_kernel, (SLABS, *double), cube, flat)(
        parts, staged, inverse_x, forward_x, *masks
    )
    parts = exchange(sent, "pencil", PENCILS)
    sent = call(middle_kernel, parts.shape)(parts, staged, edge, y_tables, z_tables)
    parts = exchange(sent, "pencil", PENCILS).reshape(flat)
    second, sent = call(back_kernel, cube, flat)(parts, masks, field, inverse_x, forward_x)
    parts = exchange(sent, "pencil", PENCILS)
    merged = call(energy_kernel, (SLABS, 3 * ROWS, GRID))(
        parts, staged, edge, field, second, y_tables, z_tables
    )
    merged = exchange(merged, "slab", SLABS).reshape(-1, GRID)
    base = right_sides.reshape(flat)
    first, second, sums = call(gram_kernel, flat, flat, (COLUMNS, GRID))(
        merged, base, mask
    )
    sums = exchange(jnp.broadcast_to(sums[None], (PENCILS, COLUMNS, GRID)), "pencil", PENCILS)
    sums = jnp.sum(sums, axis=0)
    sums = exchange(jnp.broadcast_to(sums[None], (SLABS, COLUMNS, GRID)), "slab", SLABS)
    solution, gradient = call(solve_kernel, flat, (ROWS, GRID), outputs=False)(
        sums, base, first, second
    )
    return solution.reshape(right_sides.shape), gradient.reshape(noise_var.shape)


def solution(mesh):
    return jax.shard_map(
        local,
        mesh=mesh,
        in_specs=(
            P(None, "slab", "pencil", None),
            P("pencil", "slab", None),
            P("slab", "pencil", None),
            P("slab", "pencil", None),
        ),
        out_specs=(P(None, "slab", "pencil", None), P("slab", "pencil", None)),
        check_vma=False,
    )
```

```python
import functools

import jax
import jax.numpy as jnp
import numpy as np
from jax import lax
from jax.experimental import pallas as pl
from jax.experimental.pallas import tpu as pltpu
from jax.sharding import PartitionSpec as P


GRID = 128
CELLS = GRID**3
COLUMNS = 8
SLABS = 8
PENCILS = 32
LINES = GRID // PENCILS
DEPTH = GRID // SLABS
ROWS = DEPTH * LINES
BLOCK = PENCILS * 4 * LINES
TARGETS = 4
SHIFT = 6.0
WIDTH = 8.0
F32 = jnp.float32
BF16 = jnp.bfloat16


def slot_frequencies():
    first = np.where(np.arange(PENCILS) < PENCILS // 2, 0, 1)
    return np.arange(PENCILS)[:, None] * LINES + first[:, None] + np.arange(2)[None, :]


def split_table(table):
    high = table.astype(np.float32).astype(jnp.bfloat16)
    low = (table - high.astype(np.float64)).astype(np.float32).astype(jnp.bfloat16)
    return np.stack((high, low))


@functools.cache
def tables():
    points = np.arange(GRID)
    angle = 2.0 * np.pi / GRID * (points[:, None] * points[None, :] % GRID)
    cosine, sine = np.cos(angle), np.sin(angle)
    wave = slot_frequencies().reshape(-1)
    forward_x = np.stack((cosine[wave], -sine[wave]), axis=1)
    inverse_x = np.stack((2.0 * cosine[wave], -2.0 * sine[wave]), axis=1)
    forward_x[0, 1] = cosine[GRID // 2]
    inverse_x[0, 0] = 1.0
    inverse_x[0, 1] = cosine[GRID // 2]
    forward_x = forward_x.reshape(GRID, GRID)
    inverse_x = inverse_x.reshape(GRID, GRID) / (CELLS * WIDTH)
    forward = np.block([[cosine, sine], [-sine, cosine]])
    inverse = np.block([[cosine, -sine], [sine, cosine]])
    order = (
        np.arange(2)[None, :, None] * GRID
        + np.arange(PENCILS)[:, None, None] * LINES
        + np.arange(LINES)[None, None, :]
    ).reshape(-1)
    forward_y = forward[:, order]
    inverse_y = inverse[order, :]
    return (
        split_table(forward_x),
        split_table(inverse_x),
        np.stack([split_table(t) for t in (forward_y, inverse_y)]),
        np.stack([split_table(t) for t in (forward.T, inverse.T)]),
    )


NN = (((1,), (0,)), ((), ()))
NT = (((1,), (1,)), ((), ()))
TN = (((0,), (0,)), ((), ()))


def halves(value):
    high = value.astype(BF16)
    return high, (value - high.astype(F32)).astype(BF16)


def product(left, right, dims):
    dot = functools.partial(lax.dot_general, dimension_numbers=dims, preferred_element_type=F32)
    return dot(left[0], right[0]) + (dot(left[0], right[1]) + dot(left[1], right[0]))


def pair(ref, *index):
    return ref[(*index, 0)], ref[(*index, 1)]


def lines_of(ref, line, start=0):
    return ref[:, pl.ds(start + line, DEPTH, stride=LINES), :].reshape(GRID, GRID)


def forward_x_lines(values, line, table_ref, out_ref):
    out_ref[pl.ds(line, GRID, stride=LINES), :] = product(pair(table_ref), halves(values), NT)


def start_kernel(staged_ref, table_ref, out_ref):
    for line in range(LINES):
        forward_x_lines(lines_of(staged_ref, line), line, table_ref, out_ref)


def spectrum_of(block, y_ref, z_ref):
    rows = product(pair(y_ref, 0), halves(block), NN)
    rows = jnp.concatenate((rows[:GRID], rows[GRID:]), axis=1)
    return product(halves(rows), pair(z_ref, 0), NN)


def slot_of(in_ref, slot):
    return in_ref[:, slot * 2 * LINES : (slot + 1) * 2 * LINES, :].reshape(2 * GRID, GRID)


def weighted_slots(in_ref, weights, y_ref, z_ref):
    real_weight, imag_weight, other_weight = [
        jnp.concatenate((weight, weight), axis=1) for weight in weights
    ]
    block = slot_of(in_ref, 0)
    rows = lax.broadcasted_iota(jnp.int32, block.shape, 0)
    is_real = rows % (2 * LINES) < LINES
    real = spectrum_of(jnp.where(is_real, block, 0.0), y_ref, z_ref)
    imag = spectrum_of(jnp.where(is_real, 0.0, block), y_ref, z_ref)
    other = spectrum_of(slot_of(in_ref, 1), y_ref, z_ref)
    return real_weight * real + imag_weight * imag, other_weight * other


def plane_of(staged_ref, plane):
    start = ROWS + DEPTH * plane
    return staged_ref[:, start : start + DEPTH, :].reshape(GRID, GRID)


def eigen_planes(staged_ref, edge_ref):
    first = plane_of(staged_ref, 0)
    alone = lax.axis_index("pencil") == 0
    partner = jnp.where(alone, edge_ref[...], first)
    return alone, (first, partner, plane_of(staged_ref, 1))


def middle_kernel(in_ref, staged_ref, edge_ref, y_ref, z_ref, out_ref):
    slots = weighted_slots(in_ref, eigen_planes(staged_ref, edge_ref)[1], y_ref, z_ref)
    for slot, waves in enumerate(slots):
        rows = product(halves(waves), pair(z_ref, 1), NN)
        rows = jnp.concatenate((rows[:, :GRID], rows[:, GRID:]), axis=0)
        block = product(pair(y_ref, 1), halves(rows), NN)
        out_ref[:, slot * 2 * LINES : (slot + 1) * 2 * LINES, :] = block.reshape(
            PENCILS, 2 * LINES, GRID
        )


def neighbour(step):
    return lax.rem(lax.axis_index("slab") + (SLABS + step), SLABS)


def first_back_kernel(in_ref, last_ref, inverse_ref, forward_ref, *refs):
    parts, (mask_ref, field_ref, out_ref) = refs[:SLABS], refs[SLABS:]
    for step, part in enumerate(parts):
        mask_ref[neighbour(-step)] = part[...]
    back_kernel(in_ref, mask_ref, last_ref, inverse_ref, forward_ref, field_ref, out_ref)


def back_kernel(in_ref, mask_ref, last_ref, inverse_ref, forward_ref, field_ref, out_ref):
    for line in range(LINES):
        waves = in_ref[pl.ds(line, GRID, stride=LINES), :]
        smooth = product(halves(waves), pair(inverse_ref), TN)
        seen = lines_of(mask_ref, line)
        noise = lines_of(mask_ref, line, ROWS)
        field = seen * smooth + noise * lines_of(last_ref, line)
        field_ref[:, pl.ds(line, DEPTH, stride=LINES), :] = field.reshape(SLABS, DEPTH, GRID)
        forward_x_lines(field, line, forward_ref, out_ref)


def energy_kernel(in_ref, staged_ref, edge_ref, first_ref, second_ref, y_ref, z_ref, out_ref):
    alone, planes = eigen_planes(staged_ref, edge_ref)
    share = 2.0 / (CELLS * WIDTH)
    single = jnp.where(alone, 0.5 * share, share)
    factors = (single, single, share)
    weights = [jnp.sqrt(plane * factor) for plane, factor in zip(planes, factors)]
    slots = weighted_slots(in_ref, weights, y_ref, z_ref)
    for index in range(4):
        part = index % 2 * GRID
        values = slots[index // 2][:, part : part + GRID]
        out_ref[:, index * DEPTH : (index + 1) * DEPTH, :] = values.reshape(SLABS, DEPTH, GRID)
    out_ref[:, ROWS : 2 * ROWS, :] = first_ref[...]
    out_ref[:, 2 * ROWS :, :] = second_ref[...]


def gram_kernel(in_ref, base_ref, mask_ref, first_ref, second_ref, out_ref):
    noise_ref = mask_ref.at[ROWS:, :]
    hidden = (1.0 - mask_ref[:ROWS, :]) * noise_ref[...]
    hidden_twice = hidden * noise_ref[...]
    for column in range(COLUMNS):
        source = column * 3 * ROWS
        rows = slice(column * ROWS, (column + 1) * ROWS)
        base = base_ref[rows, :]
        first_ref[rows, :] = in_ref[source + ROWS : source + 2 * ROWS, :] + hidden * base
        second_ref[rows, :] = in_ref[source + 2 * ROWS : source + 3 * ROWS, :] + hidden_twice * base
    zeroth, first, second, scaled, waves = [], [], [], [], []
    for row in range(ROWS):
        pick = pl.ds(row, COLUMNS, stride=ROWS)
        zeroth.append(base_ref[pick, :])
        first.append(first_ref[pick, :])
        second.append(second_ref[pick, :])
        scaled.append(second[-1] * noise_ref[row : row + 1, :])
        waves.append(in_ref[pl.ds(row, COLUMNS, stride=3 * ROWS), :])
    zeroth, first, second, scaled, waves = [
        halves(jnp.concatenate(parts, axis=1)) for parts in (zeroth, first, second, scaled, waves)
    ]
    out_ref[...] = jnp.zeros_like(out_ref)

    def stacked(*parts):
        return [jnp.concatenate(half, axis=0) for half in zip(*parts)]

    pairs = (
        (zeroth, stacked(zeroth, first)),
        (first, stacked(first, second)),
        (second, stacked(second, scaled)),
        (waves, waves),
    )
    start = 0
    for left, right in pairs:
        sums = product(left, right, NT)
        out_ref[:, start : start + sums.shape[1]] = sums
        start += sums.shape[1]


def solve_kernel(
    sums_ref, base_ref, first_ref, second_ref, solution_ref, gradient_ref
):
    lanes = lax.broadcasted_iota(jnp.int32, (COLUMNS, GRID), 1)
    moments = sums_ref[0]
    for slab in range(1, SLABS):
        moments = moments + sums_ref[slab]
    last = (lanes >= 5 * COLUMNS) & (lanes < 6 * COLUMNS)
    moments = moments + jnp.where(last, pltpu.roll(moments, GRID - COLUMNS, 1), 0.0)

    def moved(count):
        return moments if count == 0 else pltpu.roll(moments, count * COLUMNS % GRID, 1)

    degree = 3
    size = degree * COLUMNS
    blocks = []
    for step in range(degree):
        operator = WIDTH * moved(GRID // COLUMNS - step - 1) + SHIFT * moved(
            (GRID // COLUMNS - step) % (GRID // COLUMNS)
        )
        blocks.append(jnp.where(lanes < size, operator, moved(degree - step)))
    system = jnp.concatenate(blocks, axis=0)
    rows = lax.broadcasted_iota(jnp.int32, (size, 1), 0)
    for step in range(0, size, 2):
        upper, lower = system[step : step + 1, :], system[step + 1 : step + 2, :]
        left, right = [
            jnp.broadcast_to(system[:, lane : lane + 1], system.shape) for lane in (step, step + 1)
        ]
        top_left, low_left = left[step : step + 1], left[step + 1 : step + 2]
        top_right, low_right = right[step : step + 1], right[step + 1 : step + 2]
        scale = 1.0 / (top_left * low_right - top_right * low_left)
        new_upper = (low_right * upper - top_right * lower) * scale
        new_lower = (top_left * lower - low_left * upper) * scale
        reduced = system - left * new_upper - right * new_lower
        system = jnp.where(rows == step, new_upper, jnp.where(rows == step + 1, new_lower, reduced))
    sources = (base_ref, first_ref, second_ref)
    share = 1.0 / (COLUMNS - 1)
    weighted = jnp.zeros((ROWS, GRID), F32)
    for group in range(0, COLUMNS, TARGETS):
        totals = [jnp.zeros((ROWS, GRID), F32)] * TARGETS
        for index in range(size):
            start = index % COLUMNS * ROWS
            block = sources[index // COLUMNS][start : start + ROWS, :]
            for target in range(TARGETS):
                lane = size + group + target
                coefficient = system[index : index + 1, lane : lane + 1]
                totals[target] = totals[target] + coefficient * block
        for target, total in enumerate(totals, group):
            rows_out = slice(target * ROWS, (target + 1) * ROWS)
            solution_ref[rows_out, :] = total
            if target:
                weighted = weighted - share * (total * base_ref[rows_out, :])
            else:
                weighted = total * total
    gradient_ref[...] = 0.5 * weighted


def stage_kernel(base_ref, observed_ref, noise_ref, spectrum_ref, out_ref, mask_ref):
    seen = observed_ref[...].astype(F32)
    mask_ref[:ROWS, :] = seen
    mask_ref[ROWS:, :] = (noise_ref[...] - SHIFT) * (1.0 / WIDTH)
    low = lax.axis_index("pencil") < PENCILS // 2
    first = jnp.where(low, spectrum_ref[0], spectrum_ref[1])
    second = jnp.where(low, spectrum_ref[1], spectrum_ref[2])
    for slab in range(SLABS):
        out_ref[slab, :ROWS, :] = base_ref[slab] * seen
        for index, plane in enumerate((first, second, spectrum_ref[0])):
            start = ROWS + index * DEPTH
            out_ref[slab, start : start + DEPTH, :] = plane


def call(kernel, *shapes, inputs=pltpu.VMEM, outputs=True):
    kind = pltpu.VMEM if outputs else jax.ShapeDtypeStruct
    outs = [kind(shape, F32) for shape in shapes]
    run = pl.pallas_call(
        kernel,
        out_shape=outs if len(outs) > 1 else outs[0],
        compiler_params=pltpu.CompilerParams(vmem_limit_bytes=24 * 2**20),
    )

    def placed(*values):
        return run(*[pltpu.with_memory_space_constraint(value, inputs) for value in values])

    return placed


def exchange(values, axis, count):
    shape = values.shape
    parts = values.reshape(count, -1, shape[-1])
    return lax.all_to_all(parts, axis, 0, 0, tiled=True)


def shifted(values, step):
    ring = [(slab, (slab + step) % SLABS) for slab in range(SLABS)]
    return lax.ppermute(values, "slab", ring)


def local(right_sides, spectrum, noise_var, observed):
    forward_x, inverse_x, y_tables, z_tables = [jnp.asarray(t) for t in tables()]
    flat = (BLOCK, GRID)
    cube = (SLABS, ROWS, GRID)
    square = (ROWS, GRID)
    double = (2 * ROWS, GRID)
    staged, mask = call(
        stage_kernel, (SLABS, ROWS + 3 * DEPTH, GRID), double, inputs=pltpu.HBM
    )(
        right_sides.reshape(cube),
        observed.reshape(square),
        noise_var.reshape(square),
        spectrum,
    )
    staged = exchange(staged, "slab", SLABS)
    edge = staged[:, ROWS + 2 * DEPTH :, :].reshape(GRID, GRID)
    edge = lax.ppermute(edge, "pencil", [(PENCILS // 2, 0)])
    masks = [mask]
    for step in range(1, SLABS):
        masks.append(shifted(mask, step))

    sent = call(start_kernel, flat)(staged, forward_x)
    parts = exchange(sent, "pencil", PENCILS)
    sent = call(middle_kernel, parts.shape)(parts, staged, edge, y_tables, z_tables)
    parts = exchange(sent, "pencil", PENCILS).reshape(flat)
    masks, field, sent = call(first_back_kernel, (SLABS, *double), cube, flat)(
        parts, staged, inverse_x, forward_x, *masks
    )
    parts = exchange(sent, "pencil", PENCILS)
    sent = call(middle_kernel, parts.shape)(parts, staged, edge, y_tables, z_tables)
    parts = exchange(sent, "pencil", PENCILS).reshape(flat)
    second, sent = call(back_kernel, cube, flat)(parts, masks, field, inverse_x, forward_x)
    parts = exchange(sent, "pencil", PENCILS)
    merged = call(energy_kernel, (SLABS, 3 * ROWS, GRID))(
        parts, staged, edge, field, second, y_tables, z_tables
    )
    merged = exchange(merged, "slab", SLABS).reshape(-1, GRID)
    base = right_sides.reshape(flat)
    first, second, sums = call(gram_kernel, flat, flat, (COLUMNS, GRID))(
        merged, base, mask
    )
    sums = exchange(jnp.broadcast_to(sums[None], (PENCILS, COLUMNS, GRID)), "pencil", PENCILS)
    sums = jnp.sum(sums, axis=0)
    sums = exchange(jnp.broadcast_to(sums[None], (SLABS, COLUMNS, GRID)), "slab", SLABS)
    solution, gradient = call(solve_kernel, flat, square, outputs=False)(
        sums, base, first, second
    )
    return solution.reshape(right_sides.shape), gradient.reshape(noise_var.shape)


def solution(mesh):
    return jax.shard_map(
        local,
        mesh=mesh,
        in_specs=(
            P(None, "slab", "pencil", None),
            P("pencil", "slab", None),
            P("slab", "pencil", None),
            P("slab", "pencil", None),
        ),
        out_specs=(P(None, "slab", "pencil", None), P("slab", "pencil", None)),
        check_vma=False,
    )
```

```python
import functools

import jax
import jax.numpy as jnp
import numpy as np
from jax import lax
from jax.experimental import pallas as pl
from jax.experimental.pallas import tpu as pltpu
from jax.sharding import PartitionSpec as P


GRID = 128
CELLS = GRID**3
COLUMNS = 8
SLABS = 8
PENCILS = 32
LINES = GRID // PENCILS
DEPTH = GRID // SLABS
ROWS = DEPTH * LINES
BLOCK = PENCILS * 4 * LINES
TARGETS = 4
WIDTH = 8.0
TILE = 8
SMALLEST = 4e-7
F32 = jnp.float32
BF16 = jnp.bfloat16


def slot_frequencies():
    first = np.where(np.arange(PENCILS) < PENCILS // 2, 0, 1)
    return np.arange(PENCILS)[:, None] * LINES + first[:, None] + np.arange(2)[None, :]


def split_table(table):
    high = table.astype(np.float32).astype(jnp.bfloat16)
    low = (table - high.astype(np.float64)).astype(np.float32).astype(jnp.bfloat16)
    return np.stack((high, low))


@functools.cache
def tables():
    points = np.arange(GRID)
    angle = 2.0 * np.pi / GRID * (points[:, None] * points[None, :] % GRID)
    cosine, sine = np.cos(angle), np.sin(angle)
    wave = slot_frequencies().reshape(-1)
    forward_x = np.stack((cosine[wave], -sine[wave]), axis=1)
    inverse_x = np.stack((2.0 * cosine[wave], -2.0 * sine[wave]), axis=1)
    forward_x[0, 1] = cosine[GRID // 2]
    inverse_x[0, 0] = 1.0
    inverse_x[0, 1] = cosine[GRID // 2]
    forward_x = forward_x.reshape(GRID, GRID)
    inverse_x = inverse_x.reshape(GRID, GRID) / (CELLS * WIDTH)
    forward = np.block([[cosine, sine], [-sine, cosine]])
    inverse = np.block([[cosine, -sine], [sine, cosine]])
    order = (
        np.arange(2)[None, :, None] * GRID
        + np.arange(PENCILS)[:, None, None] * LINES
        + np.arange(LINES)[None, None, :]
    ).reshape(-1)
    forward_y = forward[:, order]
    inverse_y = inverse[order, :]
    return (
        split_table(forward_x),
        split_table(inverse_x),
        np.stack([split_table(t) for t in (forward_y, inverse_y)]),
        np.stack([split_table(t) for t in (forward.T, inverse.T)]),
    )


NN = (((1,), (0,)), ((), ()))
NT = (((1,), (1,)), ((), ()))
TN = (((0,), (0,)), ((), ()))


def halves(value):
    high = value.astype(BF16)
    return high, (value - high.astype(F32)).astype(BF16)


def product(left, right, dims):
    dot = functools.partial(lax.dot_general, dimension_numbers=dims, preferred_element_type=F32)
    return dot(left[0], right[0]) + (dot(left[0], right[1]) + dot(left[1], right[0]))


def full_product(left, right, dims):
    dot = functools.partial(lax.dot_general, dimension_numbers=dims, preferred_element_type=F32)
    return product(left, right, dims) + dot(left[1], right[1])


def pair(ref, *index):
    return ref[(*index, 0)], ref[(*index, 1)]


def lines_of(ref, line, start=0):
    return ref[:, pl.ds(start + line, DEPTH, stride=LINES), :].reshape(GRID, GRID)


def forward_x_lines(values, line, table_ref, out_ref):
    out_ref[pl.ds(line, GRID, stride=LINES), :] = product(pair(table_ref), halves(values), NT)


def start_kernel(staged_ref, table_ref, out_ref):
    for line in range(LINES):
        forward_x_lines(lines_of(staged_ref, line), line, table_ref, out_ref)


def spectrum_of(block, y_ref, z_ref):
    rows = product(pair(y_ref, 0), halves(block), NN)
    rows = jnp.concatenate((rows[:GRID], rows[GRID:]), axis=1)
    return product(halves(rows), pair(z_ref, 0), NN)


def slot_of(in_ref, slot):
    return in_ref[:, slot * 2 * LINES : (slot + 1) * 2 * LINES, :].reshape(2 * GRID, GRID)


def weighted_slots(in_ref, weights, y_ref, z_ref):
    real_weight, imag_weight, other_weight = [
        jnp.concatenate((weight, weight), axis=1) for weight in weights
    ]
    block = slot_of(in_ref, 0)
    rows = lax.broadcasted_iota(jnp.int32, block.shape, 0)
    is_real = rows % (2 * LINES) < LINES
    real = spectrum_of(jnp.where(is_real, block, 0.0), y_ref, z_ref)
    imag = spectrum_of(jnp.where(is_real, 0.0, block), y_ref, z_ref)
    other = spectrum_of(slot_of(in_ref, 1), y_ref, z_ref)
    return real_weight * real + imag_weight * imag, other_weight * other


def plane_of(staged_ref, plane):
    start = ROWS + DEPTH * plane
    return staged_ref[:, start : start + DEPTH, :].reshape(GRID, GRID)


def eigen_planes(staged_ref, edge_ref):
    first = plane_of(staged_ref, 0)
    alone = lax.axis_index("pencil") == 0
    partner = jnp.where(alone, edge_ref[...], first)
    return alone, (first, partner, plane_of(staged_ref, 1))


def middle_kernel(in_ref, staged_ref, edge_ref, y_ref, z_ref, out_ref):
    slots = weighted_slots(in_ref, eigen_planes(staged_ref, edge_ref)[1], y_ref, z_ref)
    for slot, waves in enumerate(slots):
        rows = product(halves(waves), pair(z_ref, 1), NN)
        rows = jnp.concatenate((rows[:, :GRID], rows[:, GRID:]), axis=0)
        block = product(pair(y_ref, 1), halves(rows), NN)
        out_ref[:, slot * 2 * LINES : (slot + 1) * 2 * LINES, :] = block.reshape(
            PENCILS, 2 * LINES, GRID
        )


def first_middle_kernel(in_ref, staged_ref, edge_ref, y_ref, z_ref, out_ref):
    middle_kernel(in_ref, staged_ref, edge_ref, y_ref, z_ref, out_ref)
    totals = jnp.sum(staged_ref[:, ROWS + 3 * DEPTH :, :], axis=0)
    out_ref[:, 4 * LINES :, :] = jnp.broadcast_to(totals[None], (PENCILS, TILE, GRID))


def neighbour(step):
    return lax.rem(lax.axis_index("slab") + (SLABS + step), SLABS)


def first_back_kernel(in_ref, last_ref, inverse_ref, forward_ref, *refs):
    parts, (mask_ref, shift_ref, field_ref, out_ref, flat_ref) = refs[:SLABS], refs[SLABS:]
    for step, part in enumerate(parts):
        mask_ref[neighbour(-step)] = part[...]
    totals = jnp.sum(in_ref[:, 4 * LINES :, :], axis=0)
    seen, noise, eigen = [
        jnp.sum(totals[row : row + 1, :], axis=1, keepdims=True) * (1.0 / CELLS) for row in range(3)
    ]
    shift_ref[...] = jnp.broadcast_to(seen * eigen + noise, shift_ref.shape)
    flat_ref[...] = in_ref[:, : 4 * LINES, :].reshape(BLOCK, GRID)
    back_kernel(
        flat_ref, mask_ref, shift_ref, last_ref, inverse_ref, forward_ref, field_ref, out_ref
    )


def shifted_noise(noise, shift_ref):
    return (noise - shift_ref[0:1, :]) * (1.0 / WIDTH)


def back_kernel(
    in_ref, mask_ref, shift_ref, last_ref, inverse_ref, forward_ref, field_ref, out_ref
):
    for line in range(LINES):
        waves = in_ref[pl.ds(line, GRID, stride=LINES), :]
        smooth = product(halves(waves), pair(inverse_ref), TN)
        seen = lines_of(mask_ref, line)
        noise = shifted_noise(lines_of(mask_ref, line, ROWS), shift_ref)
        field = seen * smooth + noise * lines_of(last_ref, line)
        field_ref[:, pl.ds(line, DEPTH, stride=LINES), :] = field.reshape(SLABS, DEPTH, GRID)
        forward_x_lines(field, line, forward_ref, out_ref)


def energy_kernel(in_ref, staged_ref, edge_ref, first_ref, second_ref, y_ref, z_ref, out_ref):
    alone, planes = eigen_planes(staged_ref, edge_ref)
    share = 2.0 / (CELLS * WIDTH)
    single = jnp.where(alone, 0.5 * share, share)
    factors = (single, single, share)
    weights = [jnp.sqrt(plane * factor) for plane, factor in zip(planes, factors)]
    slots = weighted_slots(in_ref, weights, y_ref, z_ref)
    for index in range(4):
        part = index % 2 * GRID
        values = slots[index // 2][:, part : part + GRID]
        out_ref[:, index * DEPTH : (index + 1) * DEPTH, :] = values.reshape(SLABS, DEPTH, GRID)
    out_ref[:, ROWS : 2 * ROWS, :] = first_ref[...]
    out_ref[:, 2 * ROWS :, :] = second_ref[...]


def gram_kernel(in_ref, base_ref, mask_ref, shift_ref, first_ref, second_ref, out_ref):
    noise = shifted_noise(mask_ref[ROWS:, :], shift_ref)
    hidden = (1.0 - mask_ref[:ROWS, :]) * noise
    hidden_twice = hidden * noise
    for column in range(COLUMNS):
        source = column * 3 * ROWS
        rows = slice(column * ROWS, (column + 1) * ROWS)
        base = base_ref[rows, :]
        first_ref[rows, :] = in_ref[source + ROWS : source + 2 * ROWS, :] + hidden * base
        second_ref[rows, :] = in_ref[source + 2 * ROWS : source + 3 * ROWS, :] + hidden_twice * base
    zeroth, first, second, scaled, waves = [], [], [], [], []
    for row in range(ROWS):
        pick = pl.ds(row, COLUMNS, stride=ROWS)
        zeroth.append(base_ref[pick, :])
        first.append(first_ref[pick, :])
        second.append(second_ref[pick, :])
        scaled.append(second[-1] * noise[row : row + 1, :])
        waves.append(in_ref[pl.ds(row, COLUMNS, stride=3 * ROWS), :])
    zeroth, first, second, scaled, waves = [
        halves(jnp.concatenate(parts, axis=1)) for parts in (zeroth, first, second, scaled, waves)
    ]
    out_ref[...] = jnp.zeros_like(out_ref)

    def stacked(*parts):
        return [jnp.concatenate(half, axis=0) for half in zip(*parts)]

    pairs = (
        (zeroth, stacked(zeroth, first)),
        (first, stacked(first, second)),
        (second, stacked(second, scaled)),
        (waves, waves),
    )
    start = 0
    for left, right in pairs:
        sums = full_product(left, right, NT)
        out_ref[:, start : start + sums.shape[1]] = sums
        start += sums.shape[1]


def solve_kernel(
    sums_ref, shift_ref, base_ref, first_ref, second_ref, solution_ref, gradient_ref
):
    lanes = lax.broadcasted_iota(jnp.int32, (COLUMNS, GRID), 1)
    moments = sums_ref[0]
    for slab in range(1, SLABS):
        moments = moments + sums_ref[slab]
    last = (lanes >= 5 * COLUMNS) & (lanes < 6 * COLUMNS)
    moments = moments + jnp.where(last, pltpu.roll(moments, GRID - COLUMNS, 1), 0.0)

    def moved(count):
        return moments if count == 0 else pltpu.roll(moments, count * COLUMNS % GRID, 1)

    degree = 3
    size = degree * COLUMNS
    blocks = []
    for step in range(degree):
        operator = WIDTH * moved(GRID // COLUMNS - step - 1) + shift_ref[...] * moved(
            (GRID // COLUMNS - step) % (GRID // COLUMNS)
        )
        blocks.append(jnp.where(lanes < size, operator, moved(degree - step)))
    system = jnp.concatenate(blocks, axis=0)
    rows = lax.broadcasted_iota(jnp.int32, (size, 1), 0)
    given = system
    for step in range(0, size, 2):
        upper, lower = system[step : step + 1, :], system[step + 1 : step + 2, :]
        left, right = [
            jnp.broadcast_to(system[:, lane : lane + 1], system.shape) for lane in (step, step + 1)
        ]
        top_left, low_left = left[step : step + 1], left[step + 1 : step + 2]
        top_right, low_right = right[step : step + 1], right[step + 1 : step + 2]
        area = top_left * low_right - top_right * low_left
        top_limit = SMALLEST * given[step : step + 1, step : step + 1]
        low_limit = SMALLEST * given[step + 1 : step + 2, step + 1 : step + 2]
        apart = (top_left > top_limit) & (area > low_limit * top_left)
        scale = jnp.where(apart, 1.0 / area, 0.0)
        new_upper = (low_right * upper - top_right * lower) * scale
        new_lower = (top_left * lower - low_left * upper) * scale
        reduced = system - left * new_upper - right * new_lower
        system = jnp.where(rows == step, new_upper, jnp.where(rows == step + 1, new_lower, reduced))
    sources = (base_ref, first_ref, second_ref)
    share = 1.0 / (COLUMNS - 1)
    weighted = jnp.zeros((ROWS, GRID), F32)
    for group in range(0, COLUMNS, TARGETS):
        totals = [jnp.zeros((ROWS, GRID), F32)] * TARGETS
        for index in range(size):
            start = index % COLUMNS * ROWS
            block = sources[index // COLUMNS][start : start + ROWS, :]
            for target in range(TARGETS):
                lane = size + group + target
                coefficient = system[index : index + 1, lane : lane + 1]
                totals[target] = totals[target] + coefficient * block
        for target, total in enumerate(totals, group):
            rows_out = slice(target * ROWS, (target + 1) * ROWS)
            solution_ref[rows_out, :] = total
            if target:
                weighted = weighted - share * (total * base_ref[rows_out, :])
            else:
                weighted = total * total
    gradient_ref[...] = 0.5 * weighted


def stage_kernel(base_ref, observed_ref, noise_ref, spectrum_ref, out_ref, mask_ref):
    seen = observed_ref[...].astype(F32)
    mask_ref[:ROWS, :] = seen
    mask_ref[ROWS:, :] = noise_ref[...]
    low = lax.axis_index("pencil") < PENCILS // 2
    first = jnp.where(low, spectrum_ref[0], spectrum_ref[1])
    second = jnp.where(low, spectrum_ref[1], spectrum_ref[2])
    totals = [
        jnp.sum(values, axis=0, keepdims=True)
        for values in (seen, noise_ref[...], spectrum_ref[...].reshape(-1, GRID))
    ]
    totals = jnp.concatenate((*totals, jnp.zeros((TILE - 3, GRID), F32)), axis=0)
    for slab in range(SLABS):
        out_ref[slab, :ROWS, :] = base_ref[slab] * seen
        out_ref[slab, ROWS + 3 * DEPTH :, :] = totals
        for index, plane in enumerate((first, second, spectrum_ref[0])):
            start = ROWS + index * DEPTH
            out_ref[slab, start : start + DEPTH, :] = plane


def call(kernel, *shapes, inputs=pltpu.VMEM, outputs=True, scratch=()):
    kind = pltpu.VMEM if outputs else jax.ShapeDtypeStruct
    outs = [kind(shape, F32) for shape in shapes]
    run = pl.pallas_call(
        kernel,
        out_shape=outs if len(outs) > 1 else outs[0],
        scratch_shapes=scratch,
        compiler_params=pltpu.CompilerParams(vmem_limit_bytes=24 * 2**20),
    )

    def placed(*values):
        return run(*[pltpu.with_memory_space_constraint(value, inputs) for value in values])

    return placed


def exchange(values, axis, count):
    shape = values.shape
    parts = values.reshape(count, -1, shape[-1])
    return lax.all_to_all(parts, axis, 0, 0, tiled=True)


def shifted(values, step):
    ring = [(slab, (slab + step) % SLABS) for slab in range(SLABS)]
    return lax.ppermute(values, "slab", ring)


def local(right_sides, spectrum, noise_var, observed):
    forward_x, inverse_x, y_tables, z_tables = [jnp.asarray(t) for t in tables()]
    flat = (BLOCK, GRID)
    cube = (SLABS, ROWS, GRID)
    square = (ROWS, GRID)
    double = (2 * ROWS, GRID)
    staged, mask = call(
        stage_kernel, (SLABS, ROWS + 3 * DEPTH + TILE, GRID), double, inputs=pltpu.HBM
    )(
        right_sides.reshape(cube),
        observed.reshape(square),
        noise_var.reshape(square),
        spectrum,
    )
    staged = exchange(staged, "slab", SLABS)
    start = ROWS + 2 * DEPTH
    edge = staged[:, start : start + DEPTH, :].reshape(GRID, GRID)
    edge = lax.ppermute(edge, "pencil", [(PENCILS // 2, 0)])
    masks = [mask]
    for step in range(1, SLABS):
        masks.append(shifted(mask, step))

    sent = call(start_kernel, flat)(staged, forward_x)
    parts = exchange(sent, "pencil", PENCILS)
    sent = call(first_middle_kernel, (PENCILS, 4 * LINES + TILE, GRID))(
        parts, staged, edge, y_tables, z_tables
    )
    parts = exchange(sent, "pencil", PENCILS)
    tile = (TILE, GRID)
    masks, shift, field, sent = call(
        first_back_kernel, (SLABS, *double), tile, cube, flat, scratch=(pltpu.VMEM(flat, F32),)
    )(parts, staged, inverse_x, forward_x, *masks)
    parts = exchange(sent, "pencil", PENCILS)
    sent = call(middle_kernel, parts.shape)(parts, staged, edge, y_tables, z_tables)
    parts = exchange(sent, "pencil", PENCILS).reshape(flat)
    second, sent = call(back_kernel, cube, flat)(
        parts, masks, shift, field, inverse_x, forward_x
    )
    parts = exchange(sent, "pencil", PENCILS)
    merged = call(energy_kernel, (SLABS, 3 * ROWS, GRID))(
        parts, staged, edge, field, second, y_tables, z_tables
    )
    merged = exchange(merged, "slab", SLABS).reshape(-1, GRID)
    base = right_sides.reshape(flat)
    first, second, sums = call(gram_kernel, flat, flat, (COLUMNS, GRID))(
        merged, base, mask, shift
    )
    sums = exchange(jnp.broadcast_to(sums[None], (PENCILS, COLUMNS, GRID)), "pencil", PENCILS)
    sums = jnp.sum(sums, axis=0)
    sums = exchange(jnp.broadcast_to(sums[None], (SLABS, COLUMNS, GRID)), "slab", SLABS)
    solution, gradient = call(solve_kernel, flat, square, outputs=False)(
        sums, shift, base, first, second
    )
    return solution.reshape(right_sides.shape), gradient.reshape(noise_var.shape)


def solution(mesh):
    return jax.shard_map(
        local,
        mesh=mesh,
        in_specs=(
            P(None, "slab", "pencil", None),
            P("pencil", "slab", None),
            P("slab", "pencil", None),
            P("slab", "pencil", None),
        ),
        out_specs=(P(None, "slab", "pencil", None), P("slab", "pencil", None)),
        check_vma=False,
    )
```

```python
import functools

import jax
import jax.numpy as jnp
import numpy as np
from jax import lax
from jax.experimental import pallas as pl
from jax.experimental.pallas import tpu as pltpu
from jax.sharding import PartitionSpec as P


GRID = 128
CELLS = GRID**3
COLUMNS = 8
SLABS = 8
PENCILS = 32
LINES = GRID // PENCILS
DEPTH = GRID // SLABS
ROWS = DEPTH * LINES
BLOCK = PENCILS * 4 * LINES
TARGETS = 2
WIDTH = 8.0
TILE = 8
SMALLEST = 4e-7
F32 = jnp.float32
BF16 = jnp.bfloat16


def slot_frequencies():
    first = np.where(np.arange(PENCILS) < PENCILS // 2, 0, 1)
    return np.arange(PENCILS)[:, None] * LINES + first[:, None] + np.arange(2)[None, :]


def split_table(table):
    high = table.astype(np.float32).astype(jnp.bfloat16)
    low = (table - high.astype(np.float64)).astype(np.float32).astype(jnp.bfloat16)
    return np.stack((high, low))


@functools.cache
def tables():
    points = np.arange(GRID)
    angle = 2.0 * np.pi / GRID * (points[:, None] * points[None, :] % GRID)
    cosine, sine = np.cos(angle), np.sin(angle)
    wave = slot_frequencies().reshape(-1)
    forward_x = np.stack((cosine[wave], -sine[wave]), axis=1)
    inverse_x = np.stack((2.0 * cosine[wave], -2.0 * sine[wave]), axis=1)
    forward_x[0, 1] = cosine[GRID // 2]
    inverse_x[0, 0] = 1.0
    inverse_x[0, 1] = cosine[GRID // 2]
    forward_x = forward_x.reshape(GRID, GRID)
    inverse_x = inverse_x.reshape(GRID, GRID) / (CELLS * WIDTH)
    forward = np.block([[cosine, sine], [-sine, cosine]])
    inverse = np.block([[cosine, -sine], [sine, cosine]])
    order = (
        np.arange(2)[None, :, None] * GRID
        + np.arange(PENCILS)[:, None, None] * LINES
        + np.arange(LINES)[None, None, :]
    ).reshape(-1)
    forward_y = forward[:, order]
    inverse_y = inverse[order, :]
    return (
        split_table(forward_x),
        split_table(inverse_x),
        np.stack([split_table(t) for t in (forward_y, inverse_y)]),
        np.stack([split_table(t) for t in (forward.T, inverse.T)]),
    )


NN = (((1,), (0,)), ((), ()))
NT = (((1,), (1,)), ((), ()))
TN = (((0,), (0,)), ((), ()))


def halves(value):
    high = value.astype(BF16)
    return high, (value - high.astype(F32)).astype(BF16)


def product(left, right, dims):
    dot = functools.partial(lax.dot_general, dimension_numbers=dims, preferred_element_type=F32)
    return dot(left[0], right[0]) + (dot(left[0], right[1]) + dot(left[1], right[0]))


def pair(ref, *index):
    return ref[(*index, 0)], ref[(*index, 1)]


def lines_of(ref, line, start=0):
    return ref[:, pl.ds(start + line, DEPTH, stride=LINES), :].reshape(GRID, GRID)


def forward_x_lines(values, line, table_ref, out_ref):
    out_ref[pl.ds(line, GRID, stride=LINES), :] = product(pair(table_ref), halves(values), NT)


def start_kernel(staged_ref, table_ref, out_ref):
    for line in range(LINES):
        forward_x_lines(lines_of(staged_ref, line), line, table_ref, out_ref)


def spectrum_of(block, y_ref, z_ref):
    rows = product(pair(y_ref, 0), halves(block), NN)
    rows = jnp.concatenate((rows[:GRID], rows[GRID:]), axis=1)
    return product(halves(rows), pair(z_ref, 0), NN)


def slot_of(in_ref, slot):
    return in_ref[:, slot * 2 * LINES : (slot + 1) * 2 * LINES, :].reshape(2 * GRID, GRID)


def weighted_slots(in_ref, weights, y_ref, z_ref):
    real_weight, imag_weight, other_weight = [
        jnp.concatenate((weight, weight), axis=1) for weight in weights
    ]
    block = slot_of(in_ref, 0)
    rows = lax.broadcasted_iota(jnp.int32, block.shape, 0)
    is_real = rows % (2 * LINES) < LINES
    real = spectrum_of(jnp.where(is_real, block, 0.0), y_ref, z_ref)
    imag = spectrum_of(jnp.where(is_real, 0.0, block), y_ref, z_ref)
    other = spectrum_of(slot_of(in_ref, 1), y_ref, z_ref)
    return real_weight * real + imag_weight * imag, other_weight * other


def plane_of(staged_ref, plane):
    start = ROWS + DEPTH * plane
    return staged_ref[:, start : start + DEPTH, :].reshape(GRID, GRID)


def eigen_planes(staged_ref, edge_ref):
    first = plane_of(staged_ref, 0)
    alone = lax.axis_index("pencil") == 0
    partner = jnp.where(alone, edge_ref[...], first)
    return alone, (first, partner, plane_of(staged_ref, 1))


def middle_kernel(in_ref, staged_ref, edge_ref, y_ref, z_ref, out_ref):
    slots = weighted_slots(in_ref, eigen_planes(staged_ref, edge_ref)[1], y_ref, z_ref)
    for slot, waves in enumerate(slots):
        rows = product(halves(waves), pair(z_ref, 1), NN)
        rows = jnp.concatenate((rows[:, :GRID], rows[:, GRID:]), axis=0)
        block = product(pair(y_ref, 1), halves(rows), NN)
        out_ref[:, slot * 2 * LINES : (slot + 1) * 2 * LINES, :] = block.reshape(
            PENCILS, 2 * LINES, GRID
        )


def first_middle_kernel(in_ref, staged_ref, edge_ref, y_ref, z_ref, out_ref):
    middle_kernel(in_ref, staged_ref, edge_ref, y_ref, z_ref, out_ref)
    totals = jnp.sum(staged_ref[:, ROWS + 3 * DEPTH :, :], axis=0)
    out_ref[:, 4 * LINES :, :] = jnp.broadcast_to(totals[None], (PENCILS, TILE, GRID))


def neighbour(step):
    return lax.rem(lax.axis_index("slab") + (SLABS + step), SLABS)


def first_back_kernel(in_ref, last_ref, inverse_ref, forward_ref, *refs):
    parts, (mask_ref, shift_ref, field_ref, out_ref, flat_ref) = refs[:SLABS], refs[SLABS:]
    for step, part in enumerate(parts):
        mask_ref[neighbour(-step)] = part[...]
    totals = jnp.sum(in_ref[:, 4 * LINES :, :], axis=0)
    seen, noise, eigen = [
        jnp.sum(totals[row : row + 1, :], axis=1, keepdims=True) * (1.0 / CELLS) for row in range(3)
    ]
    shift_ref[...] = jnp.broadcast_to(seen * eigen + noise, shift_ref.shape)
    flat_ref[...] = in_ref[:, : 4 * LINES, :].reshape(BLOCK, GRID)
    back_kernel(
        flat_ref, mask_ref, shift_ref, last_ref, inverse_ref, forward_ref, field_ref, out_ref
    )


def shifted_noise(noise, shift_ref):
    return (noise - shift_ref[0:1, :]) * (1.0 / WIDTH)


def back_kernel(
    in_ref, mask_ref, shift_ref, last_ref, inverse_ref, forward_ref, field_ref, out_ref
):
    for line in range(LINES):
        waves = in_ref[pl.ds(line, GRID, stride=LINES), :]
        smooth = product(halves(waves), pair(inverse_ref), TN)
        seen = lines_of(mask_ref, line)
        noise = shifted_noise(lines_of(mask_ref, line, ROWS), shift_ref)
        field = seen * smooth + noise * lines_of(last_ref, line)
        field_ref[:, pl.ds(line, DEPTH, stride=LINES), :] = field.reshape(SLABS, DEPTH, GRID)
        forward_x_lines(field, line, forward_ref, out_ref)


def energy_kernel(in_ref, staged_ref, edge_ref, first_ref, second_ref, y_ref, z_ref, out_ref):
    alone, planes = eigen_planes(staged_ref, edge_ref)
    share = 2.0 / (CELLS * WIDTH)
    single = jnp.where(alone, 0.5 * share, share)
    factors = (single, single, share)
    weights = [jnp.sqrt(plane * factor) for plane, factor in zip(planes, factors)]
    slots = weighted_slots(in_ref, weights, y_ref, z_ref)
    for index in range(4):
        part = index % 2 * GRID
        values = slots[index // 2][:, part : part + GRID]
        out_ref[:, index * DEPTH : (index + 1) * DEPTH, :] = values.reshape(SLABS, DEPTH, GRID)
    out_ref[:, ROWS : 2 * ROWS, :] = first_ref[...]
    out_ref[:, 2 * ROWS :, :] = second_ref[...]


def gram_kernel(in_ref, base_ref, mask_ref, shift_ref, first_ref, second_ref, out_ref):
    noise = shifted_noise(mask_ref[ROWS:, :], shift_ref)
    hidden = (1.0 - mask_ref[:ROWS, :]) * noise
    hidden_twice = hidden * noise
    for column in range(COLUMNS):
        source = column * 3 * ROWS
        rows = slice(column * ROWS, (column + 1) * ROWS)
        base = base_ref[rows, :]
        first_ref[rows, :] = in_ref[source + ROWS : source + 2 * ROWS, :] + hidden * base
        second_ref[rows, :] = in_ref[source + 2 * ROWS : source + 3 * ROWS, :] + hidden_twice * base
    zeroth, first, second, scaled, waves = [], [], [], [], []
    for row in range(ROWS):
        pick = pl.ds(row, COLUMNS, stride=ROWS)
        zeroth.append(base_ref[pick, :])
        first.append(first_ref[pick, :])
        second.append(second_ref[pick, :])
        scaled.append(second[-1] * noise[row : row + 1, :])
        waves.append(in_ref[pl.ds(row, COLUMNS, stride=3 * ROWS), :])
    zeroth, first, second, scaled, waves = [
        halves(jnp.concatenate(parts, axis=1)) for parts in (zeroth, first, second, scaled, waves)
    ]
    out_ref[...] = jnp.zeros_like(out_ref)

    def stacked(*parts):
        return [jnp.concatenate(half, axis=0) for half in zip(*parts)]

    pairs = (
        (zeroth, stacked(zeroth, first)),
        (first, stacked(first, second)),
        (second, stacked(second, scaled)),
        (waves, waves),
    )
    start = 0
    for left, right in pairs:
        sums = product(left, right, NT)
        rest = left[1].astype(F32)
        rest = jnp.sum(rest * rest, axis=1, keepdims=True)
        row, lane = [lax.broadcasted_iota(jnp.int32, sums.shape, axis) for axis in range(2)]
        sums = sums + jnp.where(row == lane, rest, 0.0)
        out_ref[:, start : start + sums.shape[1]] = sums
        start += sums.shape[1]


def solve_kernel(
    sums_ref, shift_ref, base_ref, first_ref, second_ref, solution_ref, gradient_ref
):
    lanes = lax.broadcasted_iota(jnp.int32, (COLUMNS, GRID), 1)
    moments = sums_ref[0]
    for slab in range(1, SLABS):
        moments = moments + sums_ref[slab]
    last = (lanes >= 5 * COLUMNS) & (lanes < 6 * COLUMNS)
    moments = moments + jnp.where(last, pltpu.roll(moments, GRID - COLUMNS, 1), 0.0)

    def moved(count):
        return moments if count == 0 else pltpu.roll(moments, count * COLUMNS % GRID, 1)

    degree = 3
    size = degree * COLUMNS
    blocks = []
    for step in range(degree):
        operator = WIDTH * moved(GRID // COLUMNS - step - 1) + shift_ref[...] * moved(
            (GRID // COLUMNS - step) % (GRID // COLUMNS)
        )
        blocks.append(jnp.where(lanes < size, operator, moved(degree - step)))
    system = jnp.concatenate(blocks, axis=0)
    rows = lax.broadcasted_iota(jnp.int32, (size, 1), 0)
    given = system
    for step in range(0, size, 2):
        upper, lower = system[step : step + 1, :], system[step + 1 : step + 2, :]
        left, right = [
            jnp.broadcast_to(system[:, lane : lane + 1], system.shape) for lane in (step, step + 1)
        ]
        top_left, low_left = left[step : step + 1], left[step + 1 : step + 2]
        top_right, low_right = right[step : step + 1], right[step + 1 : step + 2]
        area = top_left * low_right - top_right * low_left
        top_limit = SMALLEST * given[step : step + 1, step : step + 1]
        low_limit = SMALLEST * given[step + 1 : step + 2, step + 1 : step + 2]
        apart = (top_left > top_limit) & (area > low_limit * top_left)
        scale = jnp.where(apart, 1.0 / area, 0.0)
        new_upper = (low_right * upper - top_right * lower) * scale
        new_lower = (top_left * lower - low_left * upper) * scale
        reduced = system - left * new_upper - right * new_lower
        system = jnp.where(rows == step, new_upper, jnp.where(rows == step + 1, new_lower, reduced))
    sources = (base_ref, first_ref, second_ref)
    share = 1.0 / (COLUMNS - 1)
    weighted = jnp.zeros((ROWS, GRID), F32)
    for group in range(0, COLUMNS, TARGETS):
        totals = [jnp.zeros((ROWS, GRID), F32)] * TARGETS
        for index in range(size):
            start = index % COLUMNS * ROWS
            block = sources[index // COLUMNS][start : start + ROWS, :]
            for target in range(TARGETS):
                lane = size + group + target
                coefficient = system[index : index + 1, lane : lane + 1]
                totals[target] = totals[target] + coefficient * block
        for target, total in enumerate(totals, group):
            rows_out = slice(target * ROWS, (target + 1) * ROWS)
            solution_ref[rows_out, :] = total
            if target:
                weighted = weighted - share * (total * base_ref[rows_out, :])
            else:
                weighted = total * total
    gradient_ref[...] = 0.5 * weighted


def stage_kernel(base_ref, observed_ref, noise_ref, spectrum_ref, out_ref, mask_ref):
    seen = observed_ref[...].astype(F32)
    mask_ref[:ROWS, :] = seen
    mask_ref[ROWS:, :] = noise_ref[...]
    low = lax.axis_index("pencil") < PENCILS // 2
    first = jnp.where(low, spectrum_ref[0], spectrum_ref[1])
    second = jnp.where(low, spectrum_ref[1], spectrum_ref[2])
    totals = [
        jnp.sum(values, axis=0, keepdims=True)
        for values in (seen, noise_ref[...], spectrum_ref[...].reshape(-1, GRID))
    ]
    totals = jnp.concatenate((*totals, jnp.zeros((TILE - 3, GRID), F32)), axis=0)
    for slab in range(SLABS):
        out_ref[slab, :ROWS, :] = base_ref[slab] * seen
        out_ref[slab, ROWS + 3 * DEPTH :, :] = totals
        for index, plane in enumerate((first, second, spectrum_ref[0])):
            start = ROWS + index * DEPTH
            out_ref[slab, start : start + DEPTH, :] = plane


def call(kernel, *shapes, inputs=pltpu.VMEM, outputs=True, scratch=()):
    kind = pltpu.VMEM if outputs else jax.ShapeDtypeStruct
    outs = [kind(shape, F32) for shape in shapes]
    run = pl.pallas_call(
        kernel,
        out_shape=outs if len(outs) > 1 else outs[0],
        scratch_shapes=scratch,
        compiler_params=pltpu.CompilerParams(vmem_limit_bytes=24 * 2**20),
    )

    def placed(*values):
        return run(*[pltpu.with_memory_space_constraint(value, inputs) for value in values])

    return placed


def exchange(values, axis, count):
    shape = values.shape
    parts = values.reshape(count, -1, shape[-1])
    return lax.all_to_all(parts, axis, 0, 0, tiled=True)


def shifted(values, step):
    ring = [(slab, (slab + step) % SLABS) for slab in range(SLABS)]
    return lax.ppermute(values, "slab", ring)


def local(right_sides, spectrum, noise_var, observed):
    forward_x, inverse_x, y_tables, z_tables = [jnp.asarray(t) for t in tables()]
    flat = (BLOCK, GRID)
    cube = (SLABS, ROWS, GRID)
    square = (ROWS, GRID)
    double = (2 * ROWS, GRID)
    staged, mask = call(
        stage_kernel, (SLABS, ROWS + 3 * DEPTH + TILE, GRID), double, inputs=pltpu.HBM
    )(
        right_sides.reshape(cube),
        observed.reshape(square),
        noise_var.reshape(square),
        spectrum,
    )
    staged = exchange(staged, "slab", SLABS)
    start = ROWS + 2 * DEPTH
    edge = staged[:, start : start + DEPTH, :].reshape(GRID, GRID)
    edge = lax.ppermute(edge, "pencil", [(PENCILS // 2, 0)])
    masks = [mask]
    for step in range(1, SLABS):
        masks.append(shifted(mask, step))

    sent = call(start_kernel, flat)(staged, forward_x)
    parts = exchange(sent, "pencil", PENCILS)
    sent = call(first_middle_kernel, (PENCILS, 4 * LINES + TILE, GRID))(
        parts, staged, edge, y_tables, z_tables
    )
    parts = exchange(sent, "pencil", PENCILS)
    tile = (TILE, GRID)
    masks, shift, field, sent = call(
        first_back_kernel, (SLABS, *double), tile, cube, flat, scratch=(pltpu.VMEM(flat, F32),)
    )(parts, staged, inverse_x, forward_x, *masks)
    parts = exchange(sent, "pencil", PENCILS)
    sent = call(middle_kernel, parts.shape)(parts, staged, edge, y_tables, z_tables)
    parts = exchange(sent, "pencil", PENCILS).reshape(flat)
    second, sent = call(back_kernel, cube, flat)(
        parts, masks, shift, field, inverse_x, forward_x
    )
    parts = exchange(sent, "pencil", PENCILS)
    merged = call(energy_kernel, (SLABS, 3 * ROWS, GRID))(
        parts, staged, edge, field, second, y_tables, z_tables
    )
    merged = exchange(merged, "slab", SLABS).reshape(-1, GRID)
    base = right_sides.reshape(flat)
    first, second, sums = call(gram_kernel, flat, flat, (COLUMNS, GRID))(
        merged, base, mask, shift
    )
    sums = exchange(jnp.broadcast_to(sums[None], (PENCILS, COLUMNS, GRID)), "pencil", PENCILS)
    sums = jnp.sum(sums, axis=0)
    sums = exchange(jnp.broadcast_to(sums[None], (SLABS, COLUMNS, GRID)), "slab", SLABS)
    solution, gradient = call(solve_kernel, flat, square, outputs=False)(
        sums, shift, base, first, second
    )
    return solution.reshape(right_sides.shape), gradient.reshape(noise_var.shape)


def solution(mesh):
    return jax.shard_map(
        local,
        mesh=mesh,
        in_specs=(
            P(None, "slab", "pencil", None),
            P("pencil", "slab", None),
            P("slab", "pencil", None),
            P("slab", "pencil", None),
        ),
        out_specs=(P(None, "slab", "pencil", None), P("slab", "pencil", None)),
        check_vma=False,
    )
```
